32 devices in a mesh: section: 4 (over y, x), dp: 8 (over z, core).
Axes of the slice: x: 2, y: 2, z: 4, core: 2. Of those that a mesh axis runs over, the one named last changes fastest.
Arguments:
- token_ids: int32 [4, 512], P(None, 'dp'), may hold values from 0 to 127
- embed: bfloat16 [128, 512], replicated, may hold values from -6 to 6
- weights: bfloat16 [4, 2, 512, 2048], P('section'), may hold values from -0.25 to 0.25
- variance: bfloat16 [4, 1024, 2048], P('section', 'dp'), may hold values from 9.9658966e-05 to 0.0099487305
- momentum: bfloat16 [4, 1024, 2048], P('section', 'dp'), may hold values from -4 to 4
- worker_error: bfloat16 [4, 8, 2, 512, 2048], P('section', 'dp'), may hold values from -6 to 6
- server_error: float32 [4, 1024, 2048], P('section', 'dp'), may hold values from -0.75 to 0.75
- cotangent: bfloat16 [4, 512, 512], P(None, 'dp'), may hold values from -0.75 to 0.75
Outputs:
- new_weights: bfloat16 [4, 1024, 2048], P('section', 'dp')
- new_momentum: bfloat16 [4, 1024, 2048], P('section', 'dp')
- new_worker_error: bfloat16 [4, 8, 2, 512, 2048], P('section', 'dp')
- new_server_error: float32 [4, 1024, 2048], P('section', 'dp')
The draws below stay inside these ranges and needn't reach their ends.
All inputs are finite; a program needn't handle non-finite values.
Results may differ from the reference program's by a relative error of at most 0.012.
Values may be sent and summed in bfloat16 or wider, within the bound.
No kernel may reach another device: no remote copies, remote signals or barrier semaphores. Data moves between devices by JAX's collectives and lax.ppermute only.
A program may use at most 128 MiB of HBM per device.

```python
import math
import jax
import jax.numpy as jnp
import numpy as np
from jax import lax

D = 512
HC = 2048
VW = 128
MB = 4
TOK_MB = 64
TOKENS = 512
N_SECTION = 4
N_DP = 8


def with_ends(entries, own_key, least, high):
    longest = entries.shape.index(max(entries.shape))
    spots = []
    for shift in (0, 1):
        where = [jax.random.randint(jax.random.fold_in(own_key, axis), (), 0, length) for axis, length in enumerate(entries.shape)]
        where[longest] = (where[longest] + shift) % entries.shape[longest]
        spots.append(tuple(where))
    return entries.at[spots[0]].set(least).at[spots[1]].set(high)


def with_spikes(values, stream_key, source, target, blocks, factor):
    owner, partner = [(jnp.arange(values.shape[dim]) // (values.shape[dim] // blocks)).reshape([-1 if axis == dim else 1 for axis in range(values.ndim)]) for dim in (source, target)]
    chosen = jax.random.permutation(stream_key, blocks)[partner]
    strong = (owner == chosen) | (owner == (partner + blocks // 2) % blocks)
    return jnp.where(strong, factor * values, values)


def block_scale(own_key, shape, shards, smallest, largest):
    level = 1.0
    for axis_at, parts in shards:
        draws = jax.random.uniform(jax.random.fold_in(jax.random.fold_in(own_key, 6), axis_at), (parts,), jnp.float32, smallest / len(shards), largest / len(shards))
        level = level * jnp.repeat(jnp.exp(draws), shape[axis_at] // parts).reshape((-1,) + (1,) * (len(shape) - 1 - axis_at))
    return level


def rank_table(number_of, slope):
    weights = [(1 << 20) // math.isqrt(standing ** slope) + 1 for standing in range(1, number_of + 1)]
    width = 1 + sum(weights) // (1 << 30)
    return np.cumsum(np.array([max(1, weight // width) for weight in weights]))


def skewed_ids(own_key, extent, count, slope):
    table = rank_table(count, slope)
    pick = jax.random.randint(jax.random.fold_in(own_key, 1), extent, 0, int(table[count - 1]))
    standing = jnp.searchsorted(jnp.asarray(table, jnp.int32), pick, side="right")
    return jax.random.permutation(jax.random.fold_in(own_key, 2), count)[standing].astype(jnp.int32)


def centred(key, shape, width, limit, shards=(), kind=jnp.bfloat16):
    values = width * jax.random.normal(key, shape, jnp.float32)
    if shards:
        values = values * block_scale(key, shape, shards, -0.22, 0.18)
    return jnp.clip(values, -limit, limit).astype(kind)


def heavy_noise(rng, dims, deviation, reach, shards, heavy, kind=jnp.bfloat16):
    result = deviation * jax.random.normal(rng, dims, jnp.float32)
    if shards:
        result = result * block_scale(rng, dims, shards, -0.22, 0.18)
    return jnp.clip(with_spikes(result, jax.random.fold_in(rng, 3), *heavy), -reach, reach).astype(kind)


def setup_inputs(seed: int = 0) -> dict:
    splits = jax.random.split(jax.random.key(seed), 9)
    token_ids = with_ends(skewed_ids(splits[0], (MB, TOKENS), VW, 2), jax.random.fold_in(splits[0], 3), 0, VW - 1).astype(jnp.int32)
    embed = centred(splits[1], (VW, D), 1.0, 6.0)
    weights = centred(splits[2], (N_SECTION, 2, D, HC), D ** -0.5, 0.25, ((0, 4),))
    variance = jnp.clip(jnp.exp(math.log(0.0099487305) - 4.603446 * jax.random.uniform(splits[3], (N_SECTION, 2 * D, HC), jnp.float32) ** block_scale(splits[3], (N_SECTION, 2 * D, HC), ((0, 4), (1, 8)), -0.2, 0.2)), 9.965896606445312e-05, 0.0099487305).astype(jnp.bfloat16)
    momentum = centred(splits[4], (N_SECTION, 2 * D, HC), 0.5, 4.0, ((0, 4), (1, 8)))
    worker_error = heavy_noise(splits[5], (N_SECTION, N_DP, 2, D, HC), 0.3, 6.0, ((0, 4), (1, 8)), (1, 3, 8, 2.0))
    server_error = centred(splits[6], (N_SECTION, 2 * D, HC), 0.05, 0.75, ((0, 4), (1, 8)), jnp.float32)
    cotangent = centred(splits[7], (MB, TOKENS, D), 0.05, 0.75, ((1, 8),))
    return dict(token_ids=token_ids, embed=embed, weights=weights, variance=variance, momentum=momentum, worker_error=worker_error, server_error=server_error, cotangent=cotangent)


gelu_coef = math.sqrt(2.0 / math.pi)

def gelu_value(upper):
    inner = gelu_coef * (upper + 0.044715 * upper * upper * upper)
    return 0.5 * upper * (1.0 + jnp.tanh(inner))

def gelu_slope(upper):
    inner = gelu_coef * (upper + 0.044715 * upper * upper * upper)
    bent = jnp.tanh(inner)
    return 0.5 * (1.0 + bent) + 0.5 * upper * (1.0 - bent * bent) * gelu_coef * (1.0 + 3.0 * 0.044715 * upper * upper)

def normalize(inputs):
    values = inputs.astype(jnp.float32)
    center = lax.optimization_barrier(jnp.mean(values, axis=-1, keepdims=True))
    spread = lax.optimization_barrier(jnp.mean((values - center) * (values - center), axis=-1, keepdims=True))
    scaled = lax.rsqrt(spread + 1e-05)
    return ((values - center) * scaled, scaled)

def forward_block(inputs, first_matrix, second_matrix):
    normed, scaled = normalize(inputs)
    normed_b = normed.astype(jnp.bfloat16)
    upper = jnp.dot(normed_b, first_matrix, preferred_element_type=jnp.float32)
    hidden = gelu_value(upper).astype(jnp.bfloat16)
    mixed = lax.dot_general(hidden, second_matrix, (((1,), (1,)), ((), ())), preferred_element_type=jnp.float32)
    output = (inputs.astype(jnp.float32) + mixed).astype(jnp.bfloat16)
    return (output, normed, scaled, normed_b, upper, hidden)

def backward_block(grad_out, normed, scaled, upper, first_matrix, second_matrix):
    back_hidden = jnp.dot(grad_out, second_matrix, preferred_element_type=jnp.float32)
    back_upper = (back_hidden * gelu_slope(upper)).astype(jnp.bfloat16)
    back_normed = lax.dot_general(back_upper, first_matrix, (((1,), (1,)), ((), ())), preferred_element_type=jnp.float32)
    first_mean = lax.optimization_barrier(jnp.mean(back_normed, axis=-1, keepdims=True))
    second_mean = lax.optimization_barrier(jnp.mean(back_normed * normed, axis=-1, keepdims=True))
    grad_in = (grad_out.astype(jnp.float32) + scaled * (back_normed - first_mean - normed * second_mean)).astype(jnp.bfloat16)
    return (grad_in, back_upper)

def replica_sum(left, right):
    left_rows = left.astype(jnp.float32).reshape(MB, N_DP, TOK_MB, left.shape[-1])
    right_rows = right.astype(jnp.float32).reshape(MB, N_DP, TOK_MB, right.shape[-1])
    return jnp.einsum('mrtd,mrth->rdh', left_rows, right_rows, precision=lax.Precision.HIGHEST)

def reference(token_ids, embed, weights, variance, momentum, worker_error, server_error, cotangent):
    state = jnp.take(embed, token_ids.reshape(-1).astype(jnp.int32), axis=0)
    saved = []
    for section in range(N_SECTION):
        output, normed, scaled, normed_b, upper, hidden = forward_block(state, weights[section, 0], weights[section, 1])
        saved.append((normed, scaled, normed_b, upper, hidden))
        state = output
    grad = cotangent.reshape(-1, D)
    results = [None] * N_SECTION
    for section in range(N_SECTION - 1, -1, -1):
        normed, scaled, normed_b, upper, hidden = saved[section]
        grad_in, back_upper = backward_block(grad, normed, scaled, upper, weights[section, 0], weights[section, 1])
        gradient = jnp.stack([replica_sum(normed_b, back_upper), replica_sum(grad, hidden)], axis=1)
        shared = momentum[section].astype(jnp.float32).reshape(2, D, HC)
        combined = 0.9 * shared[None] + 0.1 * gradient + worker_error[section].astype(jnp.float32)
        worker_scale = jnp.sqrt(lax.optimization_barrier(jnp.mean(combined * combined, axis=(1, 2, 3), keepdims=True)) + 0.01)
        packed = (worker_scale * jnp.tanh(combined / worker_scale)).astype(jnp.bfloat16)
        fresh_worker = (combined - packed.astype(jnp.float32)).astype(jnp.bfloat16)
        merged = (lax.optimization_barrier(jnp.sum(packed.astype(jnp.float32), axis=0)) / N_DP).reshape(2 * D, HC) + server_error[section]
        blocks = merged.reshape(N_DP, -1)
        server_scale = jnp.sqrt(lax.optimization_barrier(jnp.mean(blocks * blocks, axis=1, keepdims=True)) + 0.01)
        server_values = (server_scale * jnp.tanh(blocks / server_scale)).astype(jnp.bfloat16)
        fresh_server = (blocks - server_values.astype(jnp.float32)).reshape(2 * D, HC)
        averaged = server_values.reshape(2 * D, HC)
        step_size = 0.01 * averaged.astype(jnp.float32) / (jnp.sqrt(variance[section].astype(jnp.float32)) + 1e-08)
        fresh_weights = (weights[section].astype(jnp.float32).reshape(2 * D, HC) - step_size).astype(jnp.bfloat16)
        results[section] = (fresh_weights, averaged, fresh_worker, fresh_server)
        grad = grad_in
    new_weights = jnp.stack([item[0] for item in results])
    new_momentum = jnp.stack([item[1] for item in results])
    new_worker_error = jnp.stack([item[2] for item in results])
    new_server_error = jnp.stack([item[3] for item in results])
    return (new_weights, new_momentum, new_worker_error, new_server_error)
```

```python
import math

import jax
import jax.numpy as jnp
from jax import lax
from jax.experimental import pallas as pl
from jax.experimental.pallas import tpu as pltpu
from jax.sharding import PartitionSpec as P


gelu_coef = math.sqrt(2.0 / math.pi)
bf16, f32 = jnp.bfloat16, jnp.float32
whole = pl.BlockSpec(memory_space=pltpu.VMEM)
scalars = pl.BlockSpec(memory_space=pltpu.SMEM)


def held(array):
    return pltpu.with_memory_space_constraint(array, pltpu.VMEM)


def call(kernel, outs, scalar_args, arrays, aliases=None, limit=8, flops=0, transcendentals=0):
    moved = sum(math.prod(a.shape) * a.dtype.itemsize for a in arrays)
    return pl.pallas_call(
        kernel,
        out_shape=[pltpu.VMEM(shape, dtype) for shape, dtype in outs],
        in_specs=[scalars] * len(scalar_args) + [whole] * len(arrays),
        out_specs=[whole] * len(outs),
        input_output_aliases={len(scalar_args) + i: o for i, o in (aliases or {}).items()},
        compiler_params=pltpu.CompilerParams(vmem_limit_bytes=limit << 20),
        cost_estimate=pl.CostEstimate(flops=flops, bytes_accessed=moved, transcendentals=transcendentals),
    )(*scalar_args, *[held(a) for a in arrays])


def across(left, right):
    return lax.dot_general(left, right, (((1,), (1,)), ((), ())), preferred_element_type=f32)


def down(left, right):
    return lax.dot_general(left, right, (((0,), (0,)), ((), ())), preferred_element_type=f32)


def normalize(inputs):
    values = inputs.astype(f32)
    center = jnp.mean(values, axis=-1, keepdims=True)
    shifted = values - center
    scaled = lax.rsqrt(jnp.mean(shifted * shifted, axis=-1, keepdims=True) + 1e-05)
    return shifted * scaled, scaled


def embed_rows(token_ids, embed):
    micro, rows = token_ids.shape
    vocab, width = embed.shape

    def kernel(ids_ref, embed_ref, out_ref):
        for m in range(micro):
            ids = ids_ref[m : m + 1, :]
            hot = (lax.broadcasted_iota(jnp.int32, (vocab, rows), 0) == ids).astype(f32).astype(bf16)
            out_ref[m * rows : (m + 1) * rows, :] = down(hot, embed_ref[...]).astype(bf16)

    return call(kernel, [((micro * rows, width), bf16)], [], [token_ids, embed])[0]


slabs = 2


def spot_of(where_ref, turn, tokens):
    return jnp.where(where_ref[7] == turn, 0, tokens)


def rows_of(ref, chunk, rows):
    return ref[...] if ref.shape[0] == rows else ref[chunk * rows : (chunk + 1) * rows, :]


def forward(where, turn, inputs, weights, saved, chunk, rows, tokens):
    width = inputs.shape[1]
    channels = weights.shape[2]
    step = channels // slabs
    outs = [((rows, width), bf16)] + [
        ((2 * tokens, width), bf16),
        ((2 * tokens, width), bf16),
        ((2 * tokens, channels), bf16),
        ((2 * tokens, channels), f32),
    ]

    def kernel(where_ref, x_ref, w_ref, *refs):
        out_ref, x_out, normed_out, hidden_out, slope_out = refs[-5:]
        place = pl.ds(pl.multiple_of(spot_of(where_ref, turn, tokens) + chunk * rows, rows), rows)
        inputs = rows_of(x_ref, chunk, rows)
        normed_b = normalize(inputs)[0].astype(bf16)
        x_out[place, :] = inputs
        normed_out[place, :] = normed_b
        total = inputs.astype(f32)
        for i in range(slabs):
            part = pl.ds(i * step, step)
            upper = jnp.dot(normed_b, w_ref[0, :, part], preferred_element_type=f32)
            square = upper * upper
            bent = jnp.tanh(gelu_coef * upper * (1.0 + 0.044715 * square))
            half = 0.5 + 0.5 * bent
            hidden = (upper * half).astype(bf16)
            hidden_out[place, part] = hidden
            slope_out[place, part] = half + 0.5 * upper * (1.0 - bent * bent) * (
                gelu_coef * (1.0 + 3.0 * 0.044715 * square)
            )
            total = total + across(hidden, w_ref[1, :, part])
        out_ref[...] = total.astype(bf16)

    got = call(
        kernel,
        outs,
        [where],
        [inputs, weights, *saved],
        {2 + i: 1 + i for i in range(len(saved))},
        flops=4 * rows * width * channels,
        transcendentals=rows * channels,
    )
    return got[0], got[1:]


def backward(where, turn, grad, weights, saved, kept, chunk, rows, tokens, last):
    width = grad.shape[1]
    channels = weights.shape[2]
    step = channels // slabs
    outs = [((2 * tokens, width), bf16), ((2 * tokens, channels), bf16)]
    if not last:
        outs = outs + [((rows, width), bf16)]

    def kernel(where_ref, grad_ref, w_ref, x_ref, slope_ref, *refs):
        refs = refs[len(kept) :]
        grad_out, upper_out = refs[:2]
        place = pl.ds(pl.multiple_of(spot_of(where_ref, turn, tokens) + chunk * rows, rows), rows)
        here = pl.ds(chunk * rows, rows)
        grad = rows_of(grad_ref, chunk, rows)
        grad_out[place, :] = grad
        total = jnp.zeros((rows, width), f32)
        for i in range(slabs):
            part = pl.ds(i * step, step)
            back_hidden = jnp.dot(grad, w_ref[1, :, part], preferred_element_type=f32)
            back_upper = (back_hidden * slope_ref[here, part]).astype(bf16)
            upper_out[place, part] = back_upper
            if not last:
                total = total + across(back_upper, w_ref[0, :, part])
        if not last:
            normed, scaled = normalize(x_ref[here, :])
            first = jnp.mean(total, axis=-1, keepdims=True)
            second = jnp.mean(total * normed, axis=-1, keepdims=True)
            refs[2][...] = (grad.astype(f32) + scaled * (total - first - normed * second)).astype(bf16)

    got = call(
        kernel,
        outs,
        [where],
        [grad, weights, *saved, *kept],
        {4 + i: i for i in range(len(kept))},
        flops=(2 if last else 4) * rows * width * channels,
    )
    return (None if last else got[2]), got[:2]


def relay(where, token_ids, embed, weights, cotangent, between):
    count = lax.axis_size("section")
    micro, per_micro = token_ids.shape
    tokens = micro * per_micro
    chunks = 2 if micro % 2 == 0 else 1
    rows = tokens // chunks
    width = embed.shape[1]
    state = [embed_rows(token_ids, embed)] * chunks
    grads = [cotangent.reshape(tokens, width)] * chunks
    saved, kept = [], []

    def passed(array, source, target):
        return lax.ppermute(array, "section", [(source, target)])

    def back(hop, c):
        nonlocal kept
        out, kept = backward(where, hop, grads[c], weights, [saved[0], saved[3]], kept, c, rows, tokens, hop == 0)
        if hop:
            grads[c] = passed(out, hop, hop - 1)

    for hop in range(count):
        for c in range(chunks):
            out, saved = forward(where, hop, state[c], weights, saved, c, rows, tokens)
            if hop + 1 < count:
                state[c] = passed(out, hop, hop + 1)
            else:
                back(hop, c)
        between(hop)
    for hop in range(count - 2, -1, -1):
        for c in range(chunks):
            back(hop, c)
        between(2 * count - 2 - hop)
    return saved[1], saved[2], kept[0], kept[1]


def along(array, pairs):
    return lax.ppermute(array, "dp", [(2 * a + c, 2 * b + c) for a, b in pairs for c in (0, 1)])


def swapped(array):
    return lax.ppermute(array, "dp", [(i, i ^ 1) for i in range(lax.axis_size("dp"))])


def known_mine(where, error, known, parts):
    owned, channels = parts[0][1].shape

    def kernel(where_ref, error_ref, *refs):
        known_out, pass_out = refs[-2:]
        refs = refs[len(known) : -2]
        z, core = where_ref[0], where_ref[1]
        for (by, _, slot), ref in zip(parts, refs):

            def fill(ref=ref, by=by, slot=slot):
                rows = pl.ds(pl.multiple_of((2 * (z + by) + core) * owned, owned), owned)
                values = ref[...]
                pass_out[slot(z)] = values
                known_out[0, z + by] = 0.9 * values.astype(f32) + error_ref[rows, :].astype(f32)

            pl.when(jnp.logical_and(z + by >= 0, z + by < 4))(fill)

    return call(
        kernel,
        [((2, 4, owned, channels), f32), ((2, owned, channels), bf16)],
        [where],
        [error, *known, *[a for _, a, _ in parts]],
        {1: 0} if known else {},
        transcendentals=0,
    )


def known_other(where, error, known, first, second):
    owned, _ = first.shape[1:]

    def kernel(where_ref, error_ref, known_ref, first_ref, second_ref, out_ref):
        z, other = where_ref[0], 1 - where_ref[1]
        two_off = jnp.where(z < 2, z + 2, z - 2)
        one_off = z ^ 1
        last = 3 - z
        for chip, ref, slot in ((z, first_ref, 0), (two_off, first_ref, 1), (one_off, second_ref, 0), (last, second_ref, 1)):
            rows = pl.ds(pl.multiple_of((2 * chip + other) * owned, owned), owned)
            out_ref[1, chip] = 0.9 * ref[slot].astype(f32) + error_ref[rows, :].astype(f32)

    return call(kernel, [(known.shape, f32)], [where], [error, known, first, second], {1: 0})[0]


def add_gradient(where, known, normed, upper, grad, hidden, width):
    _, _, owned, channels = known.shape
    tokens = normed.shape[0] // 2

    def kernel(where_ref, known_ref, normed_ref, upper_ref, grad_ref, hidden_ref, out_ref, sum_ref):
        core = where_ref[1]
        total = jnp.zeros((8, channels), f32)
        for side in (0, 1):
            parity = core if side == 0 else 1 - core
            for z in range(4):
                first = 2 * z < width // owned
                left, right = (normed_ref, upper_ref) if first else (grad_ref, hidden_ref)
                column = (2 * z + parity) * owned - (0 if first else width)
                part = left[0:tokens, pl.ds(pl.multiple_of(column, owned), owned)]
                combined = known_ref[side, z] + 0.1 * down(part, right[0:tokens, :])
                out_ref[side, z] = combined
                total = total + jnp.sum((combined * combined).reshape(owned // 8, 8, channels), axis=0)
        sum_ref[0, 0] = jnp.sum(total)

    return pl.pallas_call(
        kernel,
        out_shape=[pltpu.VMEM(known.shape, f32), jax.ShapeDtypeStruct((1, 1), f32)],
        in_specs=[scalars] + [whole] * 5,
        out_specs=[whole, scalars],
        input_output_aliases={1: 0},
        compiler_params=pltpu.CompilerParams(vmem_limit_bytes=8 << 20),
        cost_estimate=pl.CostEstimate(
            flops=2 * 8 * owned * tokens * channels, bytes_accessed=16 * 8 * owned * channels, transcendentals=0
        ),
        name="add_gradient",
    )(where, *[held(a) for a in (known, normed, upper, grad, hidden)])


def scale_of(sum_ref, count):
    scale = jnp.sqrt(jnp.full((8, 128), sum_ref[0, 0], f32) * (1.0 / count) + 0.01)[0:1, 0:1]
    return scale, 1.0 / scale


def packed_part(where, sums, combined, places):
    _, _, owned, channels = combined.shape
    count = 8 * owned * channels

    def kernel(where_ref, sum_ref, combined_ref, *outs):
        scale, inverse = scale_of(sum_ref, count)
        for i, place in enumerate(places):
            for side in (1, 0):
                values = combined_ref[side, where_ref[2 + place]]
                outs[2 * i + 1 - side][...] = (scale * jnp.tanh(values * inverse)).astype(bf16)

    return call(
        kernel,
        [((owned, channels), bf16)] * (2 * len(places)),
        [where, sums],
        [combined],
        transcendentals=2 * len(places) * owned * channels,
    )


def fresh_worker(where, sums, combined):
    _, _, owned, channels = combined.shape
    count = 8 * owned * channels

    def kernel(where_ref, sum_ref, combined_ref, out_ref):
        core = where_ref[1]
        scale, inverse = scale_of(sum_ref, count)
        for side in (0, 1):
            parity = core if side == 0 else 1 - core
            for z in range(4):
                values = combined_ref[side, z]
                packed = (scale * jnp.tanh(values * inverse)).astype(bf16)
                rows = pl.ds(pl.multiple_of((2 * z + parity) * owned, owned), owned)
                out_ref[rows, :] = (values - packed.astype(f32)).astype(bf16)

    return call(kernel, [((8 * owned, channels), bf16)], [where, sums], [combined], transcendentals=count)[0]


def added(*arrays):
    def kernel(*refs):
        total = refs[0][...].astype(f32)
        for ref in refs[1:-1]:
            total = total + ref[...].astype(f32)
        refs[-1][...] = total.astype(bf16)

    return call(kernel, [(arrays[0].shape, bf16)], [], list(arrays))[0]


def server(where, parts, error, variance, weights, replicas):
    owned, channels = error.shape
    width = weights.shape[1]

    def kernel(where_ref, error_ref, variance_ref, weights_ref, *refs):
        parts, (weights_out, momentum_out, error_out) = refs[:-3], refs[-3:]
        total = parts[0][...].astype(f32)
        for ref in parts[1:]:
            total = total + ref[...].astype(f32)
        merged = total * (1.0 / replicas) + error_ref[...]
        squares = jnp.sum((merged * merged).reshape(owned // 8, 8, channels), axis=0)
        mean = jnp.sum(squares, axis=(0, 1), keepdims=True) * (1.0 / (owned * channels))
        scale = jnp.sqrt(mean + 0.01)
        values = (scale * jnp.tanh(merged * (1.0 / scale))).astype(bf16)
        momentum_out[...] = values
        wide = values.astype(f32)
        error_out[...] = merged - wide
        start = where_ref[6]
        rows = pl.ds(pl.multiple_of(lax.rem(start, width), owned), owned)
        own = weights_ref[start // width, rows, :].astype(f32)
        step = 0.01 * wide / (jnp.sqrt(variance_ref[...].astype(f32)) + 1e-08)
        weights_out[...] = (own - step).astype(bf16)

    shape = (owned, channels)
    return call(
        kernel,
        [(shape, bf16), (shape, bf16), (shape, f32)],
        [where],
        [error, variance, weights, *parts],
        transcendentals=3 * owned * channels,
    )


def on_a_line(where, token_ids, embed, weights, variance, momentum, error, server_error, cotangent):
    replicas = lax.axis_size("dp")
    width = weights.shape[1]
    far_down, far_up = [(0, 2), (1, 3)], [(3, 1), (2, 0)]
    f2 = along(momentum, far_down)
    r2 = along(momentum, far_up)
    f3 = along(momentum, [(0, 3)])
    r3 = along(momentum, [(3, 0)])
    f1 = along(momentum, [(0, 1), (1, 2), (2, 3)])
    r1 = along(momentum, [(3, 2), (2, 1), (1, 0)])
    known, out_a = known_mine(
        where, error, [], [(0, momentum, lambda z: 0), (-2, f2, lambda z: 1), (2, r2, lambda z: 1)]
    )
    in_a = swapped(out_a)
    known, out_b = known_mine(
        where,
        error,
        [known],
        [
            (-1, f1, lambda z: jnp.where(z == 2, 1, 0)),
            (1, r1, lambda z: jnp.where(z == 1, 1, 0)),
            (-3, f3, lambda z: 1),
            (3, r3, lambda z: 1),
        ],
    )
    in_b = swapped(out_b)
    normed, hidden, grad, upper = relay(where, token_ids, embed, weights, cotangent, lambda hop: None)
    known = known_other(where, error, known, in_a, in_b)
    combined, sums = add_gradient(where, known, normed, upper, grad, hidden, width)
    far_out, far = packed_part(where, sums, combined, (0,))
    far_in = swapped(far_out)
    mid_out, mid, near_out, near, own_out, own = packed_part(where, sums, combined, (1, 2, 3))
    mid_in = swapped(mid_out)
    near_in = swapped(near_out)
    own_in = swapped(own_out)
    ends, inner, outer = [(0, 1), (3, 2)], [(1, 2), (2, 1)], [(2, 3), (1, 0)]
    a1 = along(added(far, far_in), ends)
    a2 = along(added(mid, mid_in), ends)
    a3 = along(added(near, near_in), ends)
    b2 = along(added(far, far_in, a1), inner)
    b3 = along(added(mid, mid_in, a2), inner)
    c3 = along(added(near, near_in, b2), outer)
    new_worker = fresh_worker(where, sums, combined)
    new_weights, new_momentum, new_server = server(
        where, [own, own_in, a3, b3, c3], server_error, variance, weights, replicas
    )
    return new_weights, new_momentum, new_worker, new_server


def in_general(where, token_ids, embed, weights, variance, momentum, error, server_error, cotangent):
    replicas = lax.axis_size("dp")
    width, channels = weights.shape[1:]
    owned = 2 * width // replicas
    tokens = token_ids.shape[0] * token_ids.shape[1]
    shared = lax.all_gather(momentum, "dp", axis=0, tiled=True)
    normed, hidden, grad, upper = relay(where, token_ids, embed, weights, cotangent, lambda hop: None)
    gradient = jnp.concatenate(
        [down(normed[:tokens], upper[:tokens]), down(grad[:tokens], hidden[:tokens])], axis=0
    )
    combined = 0.9 * shared.astype(f32) + 0.1 * gradient + error.astype(f32)
    worker_scale = jnp.sqrt(jnp.mean(combined * combined) + 0.01)
    packed = (worker_scale * jnp.tanh(combined / worker_scale)).astype(bf16)
    new_worker = (combined - packed.astype(f32)).astype(bf16)
    total = lax.psum_scatter(packed.astype(f32), "dp", scatter_dimension=0, tiled=True)
    merged = total / replicas + server_error
    server_scale = jnp.sqrt(jnp.mean(merged * merged) + 0.01)
    values = (server_scale * jnp.tanh(merged / server_scale)).astype(bf16)
    wide = values.astype(f32)
    start = lax.axis_index("dp") * owned
    own = lax.dynamic_slice_in_dim(weights.reshape(2 * width, channels), start, owned, 0)
    step = 0.01 * wide / (jnp.sqrt(variance.astype(f32)) + 1e-08)
    return (own.astype(f32) - step).astype(bf16), values, new_worker, merged - wide


def local(token_ids, embed, weights, variance, momentum, worker_error, server_error, cotangent):
    _, _, width, channels = weights.shape
    replicas = lax.axis_size("dp")
    rank = lax.axis_index("dp")
    z = rank // 2
    upper_half = z >= 2
    order = [jnp.where(upper_half, 0, 3), jnp.where(upper_half, 1, 2), z ^ 1, z]
    start = rank * (2 * width // replicas)
    where = jnp.stack([z, rank % 2, *order, start, lax.axis_index("section")]).astype(jnp.int32)
    plan = on_a_line if replicas == 8 else in_general
    new_weights, values, new_worker, new_server = plan(
        where,
        token_ids,
        embed,
        weights[0],
        variance[0],
        momentum[0],
        worker_error.reshape(2 * width, channels),
        server_error[0],
        cotangent,
    )
    return new_weights[None], values[None], new_worker.reshape(worker_error.shape), new_server[None]


def solution(mesh):
    in_specs = (
        P(None, "dp"),
        P(),
        P("section", None, None, None),
        P("section", "dp", None),
        P("section", "dp", None),
        P("section", "dp", None, None, None),
        P("section", "dp", None),
        P(None, "dp", None),
    )
    out_specs = (
        P("section", "dp", None),
        P("section", "dp", None),
        P("section", "dp", None, None, None),
        P("section", "dp", None),
    )
    return jax.shard_map(local, mesh=mesh, in_specs=in_specs, out_specs=out_specs, check_vma=False)
```

```python
import math

import jax
import jax.numpy as jnp
from jax import lax
from jax.experimental import pallas as pl
from jax.experimental.pallas import tpu as pltpu
from jax.sharding import PartitionSpec as P


gelu_coef = math.sqrt(2.0 / math.pi)
bf16, f32 = jnp.bfloat16, jnp.float32
whole = pl.BlockSpec(memory_space=pltpu.VMEM)
outside = pl.BlockSpec(memory_space=pl.ANY)


def held(array):
    return pltpu.with_memory_space_constraint(array, pltpu.VMEM)


def call(kernel, outs, arrays, aliases=None, limit=8, flops=0, transcendentals=0, written=(), scratch=()):
    moved = sum(math.prod(a.shape) * a.dtype.itemsize for a in arrays)
    return pl.pallas_call(
        kernel,
        out_shape=[pltpu.VMEM(shape, dtype) for shape, dtype in outs]
        + [jax.ShapeDtypeStruct(shape, dtype) for shape, dtype in written],
        in_specs=[whole] * len(arrays),
        out_specs=[whole] * len(outs) + [outside] * len(written),
        input_output_aliases=aliases or {},
        scratch_shapes=list(scratch),
        compiler_params=pltpu.CompilerParams(vmem_limit_bytes=limit << 20),
        cost_estimate=pl.CostEstimate(flops=flops, bytes_accessed=moved, transcendentals=transcendentals),
    )(*[held(a) for a in arrays])


def place_on_line():
    rank = lax.axis_index("dp")
    return rank >> 1, rank & 1


def across(left, right):
    return lax.dot_general(left, right, (((1,), (1,)), ((), ())), preferred_element_type=f32)


def down(left, right):
    return lax.dot_general(left, right, (((0,), (0,)), ((), ())), preferred_element_type=f32)


def normalize(inputs):
    values = inputs.astype(f32)
    center = jnp.mean(values, axis=-1, keepdims=True)
    shifted = values - center
    scaled = lax.rsqrt(jnp.mean(shifted * shifted, axis=-1, keepdims=True) + 1e-05)
    return shifted * scaled, scaled


def embed_rows(token_ids, embed):
    micro, rows = token_ids.shape
    vocab, width = embed.shape

    def kernel(ids_ref, embed_ref, out_ref):
        for m in range(micro):
            ids = ids_ref[m : m + 1, :]
            hot = (lax.broadcasted_iota(jnp.int32, (vocab, rows), 0) == ids).astype(f32).astype(bf16)
            out_ref[m * rows : (m + 1) * rows, :] = down(hot, embed_ref[...]).astype(bf16)

    return call(kernel, [((micro * rows, width), bf16)], [token_ids, embed])[0]


slabs = 2


def spot_of(turn, tokens):
    return jnp.where(lax.axis_index("section") == turn, 0, tokens)


def rows_of(ref, chunk, rows):
    return ref[...] if ref.shape[0] == rows else ref[chunk * rows : (chunk + 1) * rows, :]


def forward(turn, inputs, weights, saved, chunk, rows, tokens):
    width = inputs.shape[1]
    channels = weights.shape[2]
    step = channels // slabs
    outs = [((rows, width), bf16)] + [
        ((2 * tokens, width), bf16),
        ((2 * tokens, width), bf16),
        ((2 * tokens, channels), bf16),
        ((2 * tokens, channels), f32),
    ]

    def kernel(x_ref, w_ref, *refs):
        out_ref, x_out, normed_out, hidden_out, slope_out = refs[-5:]
        place = pl.ds(pl.multiple_of(spot_of(turn, tokens) + chunk * rows, rows), rows)
        inputs = rows_of(x_ref, chunk, rows)
        normed_b = normalize(inputs)[0].astype(bf16)
        x_out[place, :] = inputs
        normed_out[place, :] = normed_b
        total = inputs.astype(f32)
        for i in range(slabs):
            part = pl.ds(i * step, step)
            upper = jnp.dot(normed_b, w_ref[0, :, part], preferred_element_type=f32)
            square = upper * upper
            bent = jnp.tanh(gelu_coef * upper * (1.0 + 0.044715 * square))
            half = 0.5 + 0.5 * bent
            hidden = (upper * half).astype(bf16)
            hidden_out[place, part] = hidden
            slope_out[place, part] = half + 0.5 * upper * (1.0 - bent * bent) * (
                gelu_coef * (1.0 + 3.0 * 0.044715 * square)
            )
            total = total + across(hidden, w_ref[1, :, part])
        out_ref[...] = total.astype(bf16)

    got = call(
        kernel,
        outs,
        [inputs, weights, *saved],
        {2 + i: 1 + i for i in range(len(saved))},
        flops=4 * rows * width * channels,
        transcendentals=rows * channels,
    )
    return got[0], got[1:]


def backward(turn, grad, weights, saved, kept, chunk, rows, tokens, last):
    width = grad.shape[1]
    channels = weights.shape[2]
    step = channels // slabs
    outs = [((2 * tokens, width), bf16), ((2 * tokens, channels), bf16)]
    if not last:
        outs = outs + [((rows, width), bf16)]

    def kernel(grad_ref, w_ref, x_ref, slope_ref, *refs):
        refs = refs[len(kept) :]
        grad_out, upper_out = refs[:2]
        place = pl.ds(pl.multiple_of(spot_of(turn, tokens) + chunk * rows, rows), rows)
        here = pl.ds(chunk * rows, rows)
        grad = rows_of(grad_ref, chunk, rows)
        grad_out[place, :] = grad
        total = jnp.zeros((rows, width), f32)
        for i in range(slabs):
            part = pl.ds(i * step, step)
            back_hidden = jnp.dot(grad, w_ref[1, :, part], preferred_element_type=f32)
            back_upper = (back_hidden * slope_ref[here, part]).astype(bf16)
            upper_out[place, part] = back_upper
            if not last:
                total = total + across(back_upper, w_ref[0, :, part])
        if not last:
            normed, scaled = normalize(x_ref[here, :])
            first = jnp.mean(total, axis=-1, keepdims=True)
            second = jnp.mean(total * normed, axis=-1, keepdims=True)
            refs[2][...] = (grad.astype(f32) + scaled * (total - first - normed * second)).astype(bf16)

    got = call(
        kernel,
        outs,
        [grad, weights, *saved, *kept],
        {4 + i: i for i in range(len(kept))},
        flops=(2 if last else 4) * rows * width * channels,
    )
    return (None if last else got[2]), got[:2]


def relay(token_ids, embed, weights, cotangent):
    count = lax.axis_size("section")
    micro, per_micro = token_ids.shape
    tokens = micro * per_micro
    chunks = 2 if micro % 2 == 0 else 1
    rows = tokens // chunks
    width = embed.shape[1]
    state = [embed_rows(token_ids, embed)] * chunks
    grads = [cotangent.reshape(tokens, width)] * chunks
    saved, kept = [], []

    def passed(array, source, target):
        return lax.ppermute(array, "section", [(source, target)])

    def back(hop, c):
        nonlocal kept
        out, kept = backward(hop, grads[c], weights, [saved[0], saved[3]], kept, c, rows, tokens, hop == 0)
        if hop:
            grads[c] = passed(out, hop, hop - 1)

    for hop in range(count):
        for c in range(chunks):
            out, saved = forward(hop, state[c], weights, saved, c, rows, tokens)
            if hop + 1 < count:
                state[c] = passed(out, hop, hop + 1)
            else:
                back(hop, c)
    for hop in range(count - 2, -1, -1):
        for c in range(chunks):
            back(hop, c)
    return saved[1], saved[2], kept[0], kept[1]


def along(array, pairs):
    return lax.ppermute(array, "dp", [(2 * a + c, 2 * b + c) for a, b in pairs for c in (0, 1)])


def swapped(array):
    return lax.ppermute(array, "dp", [(i, i ^ 1) for i in range(lax.axis_size("dp"))])


def known_mine(error, known, parts):
    owned, channels = parts[0][1].shape

    def kernel(error_ref, *refs):
        known_out, pass_out = refs[-2:]
        z, core = place_on_line()
        for slot, ((by, _), ref) in enumerate(zip(parts, refs[len(known) : -2])):
            block = 2 * ((z + by) & 3) + core
            rows = pl.ds(pl.multiple_of(block * owned, owned), owned)
            values = ref[...]
            pass_out[slot] = values
            known_out[block] = 0.9 * values.astype(f32) + error_ref[rows, :].astype(f32)

    return call(
        kernel,
        [((8, owned, channels), f32), ((len(parts), owned, channels), bf16)],
        [error, *known, *[a for _, a in parts]],
        {1: 0} if known else {},
    )


def known_other(error, known, parts):
    owned, _ = known.shape[1:]

    def kernel(error_ref, known_ref, *refs):
        z, core = place_on_line()
        for (by, _, slot), ref in zip(parts, refs):
            block = 2 * ((z + by) & 3) + 1 - core
            rows = pl.ds(pl.multiple_of(block * owned, owned), owned)
            refs[-1][block] = 0.9 * ref[slot].astype(f32) + error_ref[rows, :].astype(f32)

    return call(kernel, [(known.shape, f32)], [error, known, *[a for _, a, _ in parts]], {1: 0})[0]


def add_gradient(known, normed, upper, grad, hidden):
    blocks, owned, channels = known.shape
    tokens, width = normed.shape[0] // 2, normed.shape[1]
    step = channels // 4
    per = blocks // 2

    def kernel(known_ref, normed_ref, upper_ref, grad_ref, hidden_ref, out_ref, sum_ref):
        total = jnp.zeros((8, step), f32)
        for m, (left, right) in enumerate(((normed_ref, upper_ref), (grad_ref, hidden_ref))):
            turned = left[0:tokens, :].T
            for c in range(channels // step):
                part = pl.ds(c * step, step)
                gradient = jnp.dot(turned, right[0:tokens, part], preferred_element_type=f32)
                for b in range(per):
                    block = m * per + b
                    combined = known_ref[block, :, part] + 0.1 * gradient[b * owned : (b + 1) * owned]
                    out_ref[block, :, part] = combined
                    total = total + jnp.sum((combined * combined).reshape(owned // 8, 8, step), axis=0)
        sum_ref[...] = jnp.broadcast_to(jnp.sum(total, axis=(0, 1), keepdims=True), sum_ref.shape)

    return call(
        kernel,
        [(known.shape, f32), ((8, 128), f32)],
        [known, normed, upper, grad, hidden],
        {0: 0},
        limit=12,
        flops=4 * tokens * width * channels,
    )


def scale_of(sum_ref, count):
    scale = jnp.sqrt(sum_ref[0:1, 0:1] * (1.0 / count) + 0.01)
    return scale, 1.0 / scale


def chips_in_order(z):
    upper_half = z >> 1
    return (3 - 3 * upper_half, 2 - upper_half, z ^ 1, z)


def packed_part(sums, combined, places):
    blocks, owned, channels = combined.shape
    count = blocks * owned * channels

    def kernel(sum_ref, combined_ref, *outs):
        z, core = place_on_line()
        order = chips_in_order(z)
        scale, inverse = scale_of(sum_ref, count)
        for i, place in enumerate(places):
            for j, side in enumerate((1 - core, core)):
                values = combined_ref[2 * order[place] + side]
                outs[2 * i + j][...] = (scale * jnp.tanh(values * inverse)).astype(bf16)

    return call(
        kernel,
        [((owned, channels), bf16)] * (2 * len(places)),
        [sums, combined],
        transcendentals=2 * len(places) * owned * channels,
    )


def fresh_worker(sums, combined):
    blocks, owned, channels = combined.shape
    count = blocks * owned * channels

    def kernel(sum_ref, combined_ref, out_ref, made, done):
        scale, inverse = scale_of(sum_ref, count)
        copies = []
        for b in range(blocks):
            values = combined_ref[b]
            packed = (scale * jnp.tanh(values * inverse)).astype(bf16)
            made[b] = (values - packed.astype(f32)).astype(bf16)
            copies.append(pltpu.make_async_copy(made.at[b], out_ref.at[pl.ds(b * owned, owned), :], done.at[b]))
            copies[-1].start()
        for copy in copies:
            copy.wait()

    return call(
        kernel,
        [],
        [sums, combined],
        transcendentals=count,
        written=[((blocks * owned, channels), bf16)],
        scratch=[pltpu.VMEM((blocks, owned, channels), bf16), pltpu.SemaphoreType.DMA((blocks,))],
    )[0]


def added(*arrays):
    def kernel(*refs):
        total = refs[0][...].astype(f32)
        for ref in refs[1:-1]:
            total = total + ref[...].astype(f32)
        refs[-1][...] = total.astype(bf16)

    return call(kernel, [(arrays[0].shape, bf16)], list(arrays))[0]


def server(parts, error, variance, weights, replicas):
    owned, channels = error.shape
    per = weights.shape[1] // owned
    cuts = 4 if owned % 64 == 0 else 1
    rows = owned // cuts

    def kernel(error_ref, variance_ref, weights_ref, *refs):
        parts, outs, (merged_ref, w_made, m_made, e_made, done) = refs[:-8], refs[-8:-5], refs[-5:]
        squares = jnp.zeros((8, channels), f32)
        for i in range(cuts):
            here = pl.ds(i * rows, rows)
            total = parts[0][here, :].astype(f32)
            for ref in parts[1:]:
                total = total + ref[here, :].astype(f32)
            merged = total * (1.0 / replicas) + error_ref[here, :]
            merged_ref[here, :] = merged
            squares = squares + jnp.sum((merged * merged).reshape(rows // 8, 8, channels), axis=0)
        mean = jnp.sum(squares, axis=(0, 1), keepdims=True) * (1.0 / (owned * channels))
        scale = jnp.sqrt(mean + 0.01)
        inverse = 1.0 / scale
        rank = lax.axis_index("dp")
        matrix = jnp.where(rank >= per, 1, 0)
        first = (rank - per * matrix) * owned
        copies = []
        for i in range(cuts):
            here = pl.ds(i * rows, rows)
            merged = merged_ref[here, :]
            values = (scale * jnp.tanh(merged * inverse)).astype(bf16)
            m_made[here, :] = values
            wide = values.astype(f32)
            e_made[here, :] = merged - wide
            own = weights_ref[matrix, pl.ds(pl.multiple_of(first + i * rows, rows), rows), :].astype(f32)
            step = 0.01 * wide / (jnp.sqrt(variance_ref[here, :].astype(f32)) + 1e-08)
            w_made[here, :] = (own - step).astype(bf16)
            for j, made in enumerate((w_made, m_made, e_made)):
                copies.append(pltpu.make_async_copy(made.at[here, :], outs[j].at[here, :], done.at[3 * i + j]))
                copies[-1].start()
        for copy in copies:
            copy.wait()

    shape = (owned, channels)
    return call(
        kernel,
        [],
        [error, variance, weights, *parts],
        transcendentals=3 * owned * channels,
        written=[(shape, bf16), (shape, bf16), (shape, f32)],
        scratch=[
            pltpu.VMEM(shape, f32),
            pltpu.VMEM(shape, bf16),
            pltpu.VMEM(shape, bf16),
            pltpu.VMEM(shape, f32),
            pltpu.SemaphoreType.DMA((3 * cuts,)),
        ],
    )


def on_a_line(token_ids, embed, weights, variance, momentum, error, server_error, cotangent):
    replicas = lax.axis_size("dp")
    shared = {}
    for by in (2, 3, 1):
        shared[by] = along(momentum, [(i, (i + by) % 4) for i in range(4)])
    known, out_a = known_mine(error, [], [(0, momentum), (2, shared[2])])
    in_a = swapped(out_a)
    known, out_b = known_mine(error, [known], [(1, shared[3]), (3, shared[1])])
    in_b = swapped(out_b)
    normed, hidden, grad, upper = relay(token_ids, embed, weights, cotangent)
    known = known_other(error, known, [(0, in_a, 0), (2, in_a, 1), (1, in_b, 0), (3, in_b, 1)])
    combined, sums = add_gradient(known, normed, upper, grad, hidden)
    names = ("far", "mid", "near", "own")
    made = packed_part(sums, combined, (0,)) + packed_part(sums, combined, (1, 2, 3))
    mine, other = {}, {}
    for i, name in enumerate(names):
        mine[name] = made[2 * i + 1]
        other[name] = swapped(made[2 * i])

    def summed(name, pairs, *more):
        total = added(mine[name], other[name], *more)
        return along(total, pairs)

    ends, inner, outer = [(0, 1), (3, 2)], [(1, 2), (2, 1)], [(2, 3), (1, 0)]
    a1, a2, a3 = summed("far", ends), summed("mid", ends), summed("near", ends)
    b2 = summed("far", inner, a1)
    b3 = summed("mid", inner, a2)
    c3 = summed("near", outer, b2)
    new_worker = fresh_worker(sums, combined)
    new_weights, new_momentum, new_server = server(
        [mine["own"], other["own"], a3, b3, c3], server_error, variance, weights, replicas
    )
    return new_weights, new_momentum, new_worker, new_server


def in_general(token_ids, embed, weights, variance, momentum, error, server_error, cotangent):
    replicas = lax.axis_size("dp")
    width, channels = weights.shape[1:]
    owned = 2 * width // replicas
    tokens = token_ids.shape[0] * token_ids.shape[1]
    shared = lax.all_gather(momentum, "dp", axis=0, tiled=True)
    normed, hidden, grad, upper = relay(token_ids, embed, weights, cotangent)
    gradient = jnp.concatenate(
        [down(normed[:tokens], upper[:tokens]), down(grad[:tokens], hidden[:tokens])], axis=0
    )
    combined = 0.9 * shared.astype(f32) + 0.1 * gradient + error.astype(f32)
    worker_scale = jnp.sqrt(jnp.mean(combined * combined) + 0.01)
    packed = (worker_scale * jnp.tanh(combined / worker_scale)).astype(bf16)
    new_worker = (combined - packed.astype(f32)).astype(bf16)
    total = lax.psum_scatter(packed.astype(f32), "dp", scatter_dimension=0, tiled=True)
    merged = total / replicas + server_error
    server_scale = jnp.sqrt(jnp.mean(merged * merged) + 0.01)
    values = (server_scale * jnp.tanh(merged / server_scale)).astype(bf16)
    wide = values.astype(f32)
    start = lax.axis_index("dp") * owned
    own = lax.dynamic_slice_in_dim(weights.reshape(2 * width, channels), start, owned, 0)
    step = 0.01 * wide / (jnp.sqrt(variance.astype(f32)) + 1e-08)
    return (own.astype(f32) - step).astype(bf16), values, new_worker, merged - wide


def local(token_ids, embed, weights, variance, momentum, worker_error, server_error, cotangent):
    _, _, width, channels = weights.shape
    plan = on_a_line if lax.axis_size("dp") == 8 else in_general
    new_weights, values, new_worker, new_server = plan(
        token_ids,
        embed,
        weights[0],
        variance[0],
        momentum[0],
        worker_error.reshape(2 * width, channels),
        server_error[0],
        cotangent,
    )
    return new_weights[None], values[None], new_worker.reshape(worker_error.shape), new_server[None]


def solution(mesh):
    in_specs = (
        P(None, "dp"),
        P(),
        P("section", None, None, None),
        P("section", "dp", None),
        P("section", "dp", None),
        P("section", "dp", None, None, None),
        P("section", "dp", None),
        P(None, "dp", None),
    )
    out_specs = (
        P("section", "dp", None),
        P("section", "dp", None),
        P("section", "dp", None, None, None),
        P("section", "dp", None),
    )
    return jax.shard_map(local, mesh=mesh, in_specs=in_specs, out_specs=out_specs, check_vma=False)
```

```python
import math

import jax
import jax.numpy as jnp
from jax import lax
from jax.experimental import pallas as pl
from jax.experimental.pallas import tpu as pltpu
from jax.sharding import PartitionSpec as P


gelu_coef = math.sqrt(2.0 / math.pi)
bf16, f32 = jnp.bfloat16, jnp.float32
whole = pl.BlockSpec(memory_space=pltpu.VMEM)
outside = pl.BlockSpec(memory_space=pl.ANY)


def held(array):
    return pltpu.with_memory_space_constraint(array, pltpu.VMEM)


def call(kernel, outs, arrays, aliases=None, limit=8, flops=0, transcendentals=0, written=(), scratch=(), read=()):
    moved = sum(math.prod(a.shape) * a.dtype.itemsize for a in arrays)
    return pl.pallas_call(
        kernel,
        out_shape=[pltpu.VMEM(shape, dtype) for shape, dtype in outs]
        + [jax.ShapeDtypeStruct(shape, dtype) for shape, dtype in written],
        in_specs=[outside] * len(read) + [whole] * len(arrays),
        out_specs=[whole] * len(outs) + [outside] * len(written),
        input_output_aliases=aliases or {},
        scratch_shapes=list(scratch),
        compiler_params=pltpu.CompilerParams(vmem_limit_bytes=limit << 20),
        cost_estimate=pl.CostEstimate(flops=flops, bytes_accessed=moved, transcendentals=transcendentals),
    )(*[pltpu.with_memory_space_constraint(a, pltpu.HBM) for a in read], *[held(a) for a in arrays])


def place_on_line():
    rank = lax.axis_index("dp")
    return rank >> 1, rank & 1


def across(left, right):
    return lax.dot_general(left, right, (((1,), (1,)), ((), ())), preferred_element_type=f32)


def down(left, right):
    return lax.dot_general(left, right, (((0,), (0,)), ((), ())), preferred_element_type=f32)


def normalize(inputs):
    values = inputs.astype(f32)
    center = jnp.mean(values, axis=-1, keepdims=True)
    shifted = values - center
    scaled = lax.rsqrt(jnp.mean(shifted * shifted, axis=-1, keepdims=True) + 1e-05)
    return shifted * scaled, scaled


slabs = 2
chunk_count = 2
halves = 2


def on_turn(turn):
    return pl.when(lax.axis_index("section") == turn)


def rows_of(ref, start, rows):
    return ref[...] if ref.shape[0] == rows else ref[start : start + rows, :]


def block_on(inputs, parts, weights_ref, out_ref, saved, place):
    x_out, normed_out, hidden_out, slope_out = saved
    normed_b = normalize(inputs)[0].astype(bf16)
    x_out[place, :] = inputs
    normed_out[place, :] = normed_b
    total = inputs.astype(f32)
    for part, ready in parts:
        ready(0)
        upper = jnp.dot(normed_b, weights_ref[0, :, part], preferred_element_type=f32)
        square = upper * upper
        bent = jnp.tanh(gelu_coef * upper * (1.0 + 0.044715 * square))
        half = 0.5 + 0.5 * bent
        hidden = (upper * half).astype(bf16)
        hidden_out[place, part] = hidden
        slope_out[place, part] = half + 0.5 * upper * (1.0 - bent * bent) * (
            gelu_coef * (1.0 + 3.0 * 0.044715 * square)
        )
        ready(1)
        total = total + across(hidden, weights_ref[1, :, part])
    out_ref[...] = total.astype(bf16)


def saved_shapes(tokens, width, channels):
    return [((tokens, width), bf16), ((tokens, width), bf16), ((tokens, channels), bf16), ((tokens, channels), f32)]


def enter(token_ids, embed, weights, rows):
    micro, per = token_ids.shape
    vocab, width = embed.shape
    channels = weights.shape[2]
    tokens = micro * per
    step = channels // slabs

    def kernel(ids_hbm, embed_hbm, weights_hbm, out_ref, embedded_ref, weights_ref, *rest):
        saved, (ids_ref, embed_ref, small, large) = rest[:4], rest[4:]
        first = [
            pltpu.make_async_copy(ids_hbm, ids_ref, small.at[0]),
            pltpu.make_async_copy(embed_hbm, embed_ref, small.at[1]),
        ]
        copies = {}
        for i in range(slabs):
            for m in (0, 1):
                part = pl.ds(i * step, step)
                copies[i, m] = pltpu.make_async_copy(
                    weights_hbm.at[m, :, part], weights_ref.at[m, :, part], large.at[2 * i + m]
                )

        @on_turn(0)
        def _():
            for copy in (*first, *copies.values()):
                copy.start()
            for copy in first:
                copy.wait()
            for m in range(micro):
                ids = ids_ref[m : m + 1, :]
                hot = (lax.broadcasted_iota(jnp.int32, (vocab, per), 0) == ids).astype(f32).astype(bf16)
                embedded_ref[m * per : (m + 1) * per, :] = down(hot, embed_ref[...]).astype(bf16)
            parts = [(pl.ds(i * step, step), lambda m, i=i: copies[i, m].wait()) for i in range(slabs)]
            block_on(embedded_ref[0:rows, :], parts, weights_ref, out_ref, saved, pl.ds(0, rows))

    got = call(
        kernel,
        [((rows, width), bf16), ((tokens, width), bf16), (weights.shape, bf16), *saved_shapes(tokens, width, channels)],
        [],
        read=[token_ids, embed, weights],
        flops=4 * rows * width * channels,
        scratch=[
            pltpu.VMEM(token_ids.shape, token_ids.dtype),
            pltpu.VMEM(embed.shape, embed.dtype),
            pltpu.SemaphoreType.DMA((2,)),
            pltpu.SemaphoreType.DMA((2 * slabs,)),
        ],
    )
    return got[0], got[1], got[2], got[3:]


def fetched(weights, held_weights):
    def kernel(weights_hbm, _, weights_ref, done):
        @pl.when(lax.axis_index("section") != 0)
        def _():
            copy = pltpu.make_async_copy(weights_hbm, weights_ref, done)
            copy.start()
            copy.wait()

    return call(
        kernel, [(weights.shape, bf16)], [held_weights], {1: 0}, read=[weights], scratch=[pltpu.SemaphoreType.DMA]
    )[0]


def forward(turn, inputs, weights, saved, start, rows, tokens):
    width = inputs.shape[1]
    channels = weights.shape[2]
    step = channels // slabs

    def kernel(x_ref, w_ref, *refs):
        out_ref, saved_out = refs[-5], refs[-4:]

        @on_turn(turn)
        def _():
            parts = [(pl.ds(i * step, step), lambda m: None) for i in range(slabs)]
            block_on(rows_of(x_ref, start, rows), parts, w_ref, out_ref, saved_out, pl.ds(start, rows))

    got = call(
        kernel,
        [((rows, width), bf16), *saved_shapes(tokens, width, channels)],
        [inputs, weights, *saved],
        {2 + i: 1 + i for i in range(4)},
        flops=4 * rows * width * channels,
        transcendentals=rows * channels,
    )
    return got[0], got[1:]


def backward(turn, grad, weights, saved, kept, start, rows, tokens, last):
    width = grad.shape[1]
    channels = weights.shape[2]
    step = channels // slabs
    outs = [((tokens, width), bf16), ((tokens, channels), bf16)]
    if not last:
        outs = outs + [((rows, width), bf16)]

    def kernel(grad_ref, w_ref, x_ref, slope_ref, *refs):
        refs = refs[len(kept) :]
        grad_out, upper_out = refs[:2]
        here = pl.ds(start, rows)

        @on_turn(turn)
        def _():
            grad = rows_of(grad_ref, start, rows)
            grad_out[here, :] = grad
            total = jnp.zeros((rows, width), f32)
            for i in range(slabs):
                part = pl.ds(i * step, step)
                back_hidden = jnp.dot(grad, w_ref[1, :, part], preferred_element_type=f32)
                back_upper = (back_hidden * slope_ref[here, part]).astype(bf16)
                upper_out[here, part] = back_upper
                if not last:
                    total = total + across(back_upper, w_ref[0, :, part])
            if not last:
                normed, scaled = normalize(x_ref[here, :])
                first = jnp.mean(total, axis=-1, keepdims=True)
                second = jnp.mean(total * normed, axis=-1, keepdims=True)
                refs[2][...] = (grad.astype(f32) + scaled * (total - first - normed * second)).astype(bf16)

    got = call(
        kernel,
        outs,
        [grad, weights, *saved, *kept],
        {4 + i: i for i in range(len(kept))},
        flops=(2 if last else 4) * rows * width * channels,
    )
    return (None if last else got[2]), got[:2]


def cut_up(tokens):
    count = chunk_count if tokens % 16 == 0 else 1
    units = tokens // 16 if count > 1 else 1
    lengths = [(units // count + (1 if c < units % count else 0)) * (tokens // units) for c in range(count)]
    return [(sum(lengths[:c]), lengths[c]) for c in range(count)]


def relay(token_ids, embed, weights, cotangent):
    count = lax.axis_size("section")
    tokens = token_ids.shape[0] * token_ids.shape[1]
    chunks = cut_up(tokens)
    width = embed.shape[1]
    saved, kept = [], []
    entered, embedded, here, saved = enter(token_ids, embed, weights, chunks[0][1])
    weights = fetched(weights, here)
    state = [embedded] * len(chunks)
    grads = [cotangent.reshape(tokens, width)] * len(chunks)

    def passed(array, source, target):
        return lax.ppermute(array, "section", [(source, target)])

    def back(hop, c):
        nonlocal kept
        out, kept = backward(hop, grads[c], weights, [saved[0], saved[3]], kept, *chunks[c], tokens, hop == 0)
        if hop:
            grads[c] = passed(out, hop, hop - 1)

    for hop in range(count):
        for c in range(len(chunks)):
            if hop or c:
                out, saved = forward(hop, state[c], weights, saved, *chunks[c], tokens)
            else:
                out = entered
            if hop + 1 < count:
                state[c] = passed(out, hop, hop + 1)
            else:
                back(hop, c)
    for hop in range(count - 2, -1, -1):
        for c in range(len(chunks)):
            back(hop, c)
    return saved[1], saved[2], kept[0], kept[1], weights


def along(array, pairs):
    return lax.ppermute(array, "dp", [(2 * a + c, 2 * b + c) for a, b in pairs for c in (0, 1)])


def swapped(array):
    return lax.ppermute(array, "dp", [(i, i ^ 1) for i in range(lax.axis_size("dp"))])


def known_rows(error, known, parts, mine):
    owned, channels = parts[0][1].shape[-2:]

    def kernel(error_ref, *refs):
        outs = refs[len(known) + len(parts) :]
        z, core = place_on_line()
        for (by, _, slot), ref in zip(parts, refs[len(known) :]):
            block = 2 * ((z + by) & 3) + (core if mine else 1 - core)
            rows = pl.ds(pl.multiple_of(block * owned, owned), owned)
            values = ref[...] if mine else ref[slot]
            if mine:
                outs[1][slot] = values
            outs[0][block] = 0.9 * values.astype(f32) + error_ref[rows, :].astype(f32)

    return call(
        kernel,
        [((8, owned, channels), f32)] + ([((len(parts), owned, channels), bf16)] if mine else []),
        [error, *known, *[a for _, a, _ in parts]],
        {1: 0} if known else {},
    )


def add_gradient(known, normed, upper, grad, hidden):
    blocks, owned, channels = known.shape
    rows, width = normed.shape
    step = channels // 4
    per = blocks // 2

    def kernel(known_ref, normed_ref, upper_ref, grad_ref, hidden_ref, out_ref, sum_ref):
        total = jnp.zeros((8, step), f32)
        for m, (left, right) in enumerate(((normed_ref, upper_ref), (grad_ref, hidden_ref))):
            turned = left[...].T
            for c in range(channels // step):
                part = pl.ds(c * step, step)
                gradient = jnp.dot(turned, right[:, part], preferred_element_type=f32)
                for b in range(per):
                    block = m * per + b
                    combined = known_ref[block, :, part] + 0.1 * gradient[b * owned : (b + 1) * owned]
                    out_ref[block, :, part] = combined
                    total = total + jnp.sum((combined * combined).reshape(owned // 8, 8, step), axis=0)
        sum_ref[...] = jnp.broadcast_to(jnp.sum(total, axis=(0, 1), keepdims=True), sum_ref.shape)

    return call(
        kernel,
        [(known.shape, f32), ((8, 128), f32)],
        [known, normed, upper, grad, hidden],
        {0: 0},
        limit=12,
        flops=4 * rows * width * channels,
    )


def scale_of(sum_ref, count):
    scale = jnp.sqrt(sum_ref[0:1, 0:1] * (1.0 / count) + 0.01)
    return scale, 1.0 / scale


def chips_in_order(z):
    upper_half = z >> 1
    return (3 - 3 * upper_half, 2 - upper_half, z ^ 1, z)


def packed_part(sums, combined, places):
    blocks, owned, channels = combined.shape
    count = blocks * owned * channels

    def kernel(sum_ref, combined_ref, *outs):
        z, core = place_on_line()
        order = chips_in_order(z)
        scale, inverse = scale_of(sum_ref, count)
        for i, place in enumerate(places):
            for j, side in enumerate((1 - core, core)):
                values = combined_ref[2 * order[place] + side]
                outs[2 * i + j][...] = (scale * jnp.tanh(values * inverse)).astype(bf16)

    return call(
        kernel,
        [((owned, channels), bf16)] * (2 * len(places)),
        [sums, combined],
        transcendentals=2 * len(places) * owned * channels,
    )


def fresh_worker(sums, combined):
    blocks, owned, channels = combined.shape
    count = blocks * owned * channels

    def kernel(sum_ref, combined_ref, out_ref, made, done):
        scale, inverse = scale_of(sum_ref, count)
        copies = []
        for b in range(blocks):
            values = combined_ref[b]
            packed = (scale * jnp.tanh(values * inverse)).astype(bf16)
            made[b] = (values - packed.astype(f32)).astype(bf16)
            copies.append(pltpu.make_async_copy(made.at[b], out_ref.at[pl.ds(b * owned, owned), :], done.at[b]))
            copies[-1].start()
        for copy in copies:
            copy.wait()

    return call(
        kernel,
        [],
        [sums, combined],
        transcendentals=count,
        written=[((blocks * owned, channels), bf16)],
        scratch=[pltpu.VMEM((blocks, owned, channels), bf16), pltpu.SemaphoreType.DMA((blocks,))],
    )[0]


def added(cut, count, *arrays):
    rows, channels = arrays[0].shape[0] // count, arrays[0].shape[1]

    def kernel(*refs):
        total = jnp.zeros((rows, channels), f32)
        for ref in refs[:-1]:
            total = total + rows_of(ref, cut * rows, rows).astype(f32)
        refs[-1][...] = total.astype(bf16)

    return call(kernel, [((rows, channels), bf16)], list(arrays))[0]


def prepared(mine, other, error, variance, replicas):
    def kernel(mine_ref, other_ref, error_ref, variance_ref, base_ref, rate_ref):
        base_ref[...] = (mine_ref[...].astype(f32) + other_ref[...].astype(f32)) * (1.0 / replicas) + error_ref[...]
        rate_ref[...] = 0.01 / (jnp.sqrt(variance_ref[...].astype(f32)) + 1e-08)

    return call(kernel, [(error.shape, f32), (error.shape, f32)], [mine, other, error, variance])


def server(base, rate, parts, weights, replicas):
    owned, channels = base.shape
    per = weights.shape[1] // owned
    cuts = 4 if owned % 64 == 0 else 1
    rows = owned // cuts
    flat = [a for part in parts for a in part]

    def kernel(base_ref, rate_ref, weights_ref, *refs):
        got, outs, (merged_ref, w_made, m_made, e_made, done) = refs[:-8], refs[-8:-5], refs[-5:]
        squares = jnp.zeros((8, channels), f32)
        for i in range(cuts):
            here = pl.ds(i * rows, rows)
            total = jnp.zeros((rows, channels), f32)
            at = 0
            for part in parts:
                high = part[0].shape[0]
                total = total + got[at + i * rows // high][pl.ds(i * rows % high, rows), :].astype(f32)
                at += len(part)
            merged = total * (1.0 / replicas) + base_ref[here, :]
            merged_ref[here, :] = merged
            squares = squares + jnp.sum((merged * merged).reshape(rows // 8, 8, channels), axis=0)
        mean = jnp.sum(squares, axis=(0, 1), keepdims=True) * (1.0 / (owned * channels))
        scale = jnp.sqrt(mean + 0.01)
        inverse = 1.0 / scale
        rank = lax.axis_index("dp")
        matrix = jnp.where(rank >= per, 1, 0)
        first = (rank - per * matrix) * owned
        copies = []
        for i in range(cuts):
            here = pl.ds(i * rows, rows)
            merged = merged_ref[here, :]
            values = (scale * jnp.tanh(merged * inverse)).astype(bf16)
            m_made[here, :] = values
            wide = values.astype(f32)
            e_made[here, :] = merged - wide
            own = weights_ref[matrix, pl.ds(pl.multiple_of(first + i * rows, rows), rows), :].astype(f32)
            w_made[here, :] = (own - wide * rate_ref[here, :]).astype(bf16)
            for j, made in enumerate((w_made, m_made, e_made)):
                copies.append(pltpu.make_async_copy(made.at[here, :], outs[j].at[here, :], done.at[3 * i + j]))
                copies[-1].start()
        for copy in copies:
            copy.wait()

    shape = (owned, channels)
    return call(
        kernel,
        [],
        [base, rate, weights, *flat],
        transcendentals=owned * channels,
        written=[(shape, bf16), (shape, bf16), (shape, f32)],
        scratch=[
            pltpu.VMEM(shape, f32),
            pltpu.VMEM(shape, bf16),
            pltpu.VMEM(shape, bf16),
            pltpu.VMEM(shape, f32),
            pltpu.SemaphoreType.DMA((3 * cuts,)),
        ],
    )


def turned_round(own, up, down):
    def kernel(own_ref, up_ref, lowerref, out_ref):
        z, _ = place_on_line()
        for ref, here in ((own_ref, jnp.logical_or(z == 0, z == 3)), (up_ref, z == 2), (lowerref, z == 1)):

            @pl.when(here)
            def _(ref=ref):
                out_ref[...] = ref[...]

    return call(kernel, [(own.shape, own.dtype)], [own, up, down])[0]


def on_a_line(token_ids, embed, weights, variance, momentum, error, server_error, cotangent):
    replicas = lax.axis_size("dp")
    up = along(momentum, [(i, (i + 1) % 4) for i in range(4)])
    lower = along(momentum, [(i, (i + 3) % 4) for i in range(4)])
    onward = turned_round(momentum, up, lower)
    onward = along(onward, [(0, 2), (2, 3), (3, 1), (1, 0)])
    known, out_a = known_rows(error, [], [(0, momentum, 0), (3, up, 1), (1, lower, 2)], True)
    in_a = swapped(out_a)
    known, out_b = known_rows(error, [known], [(2, onward, 0)], True)
    in_b = swapped(out_b)
    known = known_rows(error, [known], [(0, in_a, 0), (3, in_a, 1), (1, in_a, 2), (2, in_b, 0)], False)[0]
    normed, hidden, grad, upper, weights = relay(token_ids, embed, weights, cotangent)
    combined, sums = add_gradient(known, normed, upper, grad, hidden)
    names = ("far", "mid", "near", "own")
    made = packed_part(sums, combined, (0,)) + packed_part(sums, combined, (1, 2, 3))
    mine, other = {}, {}
    for i, name in enumerate(names):
        mine[name] = made[2 * i + 1]
        other[name] = swapped(made[2 * i])

    def summed(name, pairs, cut, count, *more):
        total = added(cut, count, mine[name], other[name], *more)
        return along(total, pairs)

    ends, inner, outer = [(0, 1), (3, 2)], [(1, 2), (2, 1)], [(2, 3), (1, 0)]
    both = range(halves)
    a1 = [summed("far", ends, h, halves) for h in both]
    a2 = [summed("mid", ends, h, halves) for h in both]
    a3 = [summed("near", ends, 0, 1)]
    b2 = [summed("far", inner, h, halves, a1[h]) for h in both]
    b3 = [summed("mid", inner, h, halves, a2[h]) for h in both]
    c3 = [summed("near", outer, h, halves, b2[h]) for h in both]
    new_worker = fresh_worker(sums, combined)
    base, rate = prepared(mine["own"], other["own"], server_error, variance, replicas)
    new_weights, new_momentum, new_server = server(base, rate, [a3, b3, c3], weights, replicas)
    return new_weights, new_momentum, new_worker, new_server


def in_general(token_ids, embed, weights, variance, momentum, error, server_error, cotangent):
    replicas = lax.axis_size("dp")
    width, channels = weights.shape[1:]
    owned = 2 * width // replicas
    shared = lax.all_gather(momentum, "dp", axis=0, tiled=True)
    normed, hidden, grad, upper, weights = relay(token_ids, embed, weights, cotangent)
    gradient = jnp.concatenate(
        [down(normed, upper), down(grad, hidden)], axis=0
    )
    combined = 0.9 * shared.astype(f32) + 0.1 * gradient + error.astype(f32)
    worker_scale = jnp.sqrt(jnp.mean(combined * combined) + 0.01)
    packed = (worker_scale * jnp.tanh(combined / worker_scale)).astype(bf16)
    new_worker = (combined - packed.astype(f32)).astype(bf16)
    total = lax.psum_scatter(packed.astype(f32), "dp", scatter_dimension=0, tiled=True)
    merged = total / replicas + server_error
    server_scale = jnp.sqrt(jnp.mean(merged * merged) + 0.01)
    values = (server_scale * jnp.tanh(merged / server_scale)).astype(bf16)
    wide = values.astype(f32)
    start = lax.axis_index("dp") * owned
    own = lax.dynamic_slice_in_dim(weights.reshape(2 * width, channels), start, owned, 0)
    step = 0.01 * wide / (jnp.sqrt(variance.astype(f32)) + 1e-08)
    return (own.astype(f32) - step).astype(bf16), values, new_worker, merged - wide


def local(token_ids, embed, weights, variance, momentum, worker_error, server_error, cotangent):
    _, _, width, channels = weights.shape
    plan = on_a_line if lax.axis_size("dp") == 8 else in_general
    new_weights, values, new_worker, new_server = plan(
        token_ids,
        embed,
        weights[0],
        variance[0],
        momentum[0],
        worker_error.reshape(2 * width, channels),
        server_error[0],
        cotangent,
    )
    return new_weights[None], values[None], new_worker.reshape(worker_error.shape), new_server[None]


def solution(mesh):
    in_specs = (
        P(None, "dp"),
        P(),
        P("section", None, None, None),
        P("section", "dp", None),
        P("section", "dp", None),
        P("section", "dp", None, None, None),
        P("section", "dp", None),
        P(None, "dp", None),
    )
    out_specs = (
        P("section", "dp", None),
        P("section", "dp", None),
        P("section", "dp", None, None, None),
        P("section", "dp", None),
    )
    return jax.shard_map(local, mesh=mesh, in_specs=in_specs, out_specs=out_specs, check_vma=False)
```

```python
import math

import jax
import jax.numpy as jnp
from jax import lax
from jax.experimental import pallas as pl
from jax.experimental.pallas import tpu as pltpu
from jax.sharding import PartitionSpec as P


gelu_coef = math.sqrt(2.0 / math.pi)
bf16, f32 = jnp.bfloat16, jnp.float32
whole = pl.BlockSpec(memory_space=pltpu.VMEM)
outside = pl.BlockSpec(memory_space=pl.ANY)


def held(array):
    return pltpu.with_memory_space_constraint(array, pltpu.VMEM)


def call(kernel, outs, arrays, aliases=None, limit=8, flops=0, transcendentals=0, written=(), scratch=(), read=()):
    moved = sum(math.prod(a.shape) * a.dtype.itemsize for a in arrays)
    return pl.pallas_call(
        kernel,
        out_shape=[pltpu.VMEM(shape, dtype) for shape, dtype in outs]
        + [jax.ShapeDtypeStruct(shape, dtype) for shape, dtype in written],
        in_specs=[outside] * len(read) + [whole] * len(arrays),
        out_specs=[whole] * len(outs) + [outside] * len(written),
        input_output_aliases=aliases or {},
        scratch_shapes=list(scratch),
        compiler_params=pltpu.CompilerParams(vmem_limit_bytes=limit << 20),
        cost_estimate=pl.CostEstimate(flops=flops, bytes_accessed=moved, transcendentals=transcendentals),
    )(*[pltpu.with_memory_space_constraint(a, pltpu.HBM) for a in read], *[held(a) for a in arrays])


def place_on_line():
    rank = lax.axis_index("dp")
    return rank >> 1, rank & 1


def across(left, right):
    return lax.dot_general(left, right, (((1,), (1,)), ((), ())), preferred_element_type=f32)


def down(left, right):
    return lax.dot_general(left, right, (((0,), (0,)), ((), ())), preferred_element_type=f32)


def normalize(inputs):
    values = inputs.astype(f32)
    center = jnp.mean(values, axis=-1, keepdims=True)
    shifted = values - center
    scaled = lax.rsqrt(jnp.mean(shifted * shifted, axis=-1, keepdims=True) + 1e-05)
    return shifted * scaled, scaled


slabs = 2
chunk_count = 2
halves = 2


def on_turn(turn):
    return pl.when(lax.axis_index("section") == turn)


def rows_of(ref, start, rows):
    return ref[...] if ref.shape[0] == rows else ref[start : start + rows, :]


def block_on(inputs, parts, weights_ref, out_ref, saved, place):
    x_out, normed_out, hidden_out, slope_out = saved
    normed_b = normalize(inputs)[0].astype(bf16)
    x_out[place, :] = inputs
    normed_out[place, :] = normed_b
    total = inputs.astype(f32) if out_ref is not None else None
    for part, ready in parts:
        ready(0)
        upper = jnp.dot(normed_b, weights_ref[0, :, part], preferred_element_type=f32)
        square = upper * upper
        bent = jnp.tanh(gelu_coef * upper * (1.0 + 0.044715 * square))
        half = 0.5 + 0.5 * bent
        hidden = (upper * half).astype(bf16)
        hidden_out[place, part] = hidden
        slope_out[place, part] = half + 0.5 * upper * (1.0 - bent * bent) * (
            gelu_coef * (1.0 + 3.0 * 0.044715 * square)
        )
        ready(1)
        if out_ref is not None:
            total = total + across(hidden, weights_ref[1, :, part])
    if out_ref is not None:
        out_ref[...] = total.astype(bf16)


def saved_shapes(tokens, width, channels):
    return [((tokens, width), bf16), ((tokens, width), bf16), ((tokens, channels), bf16), ((tokens, channels), f32)]


def enter(token_ids, embed, weights, rows):
    micro, per = token_ids.shape
    vocab, width = embed.shape
    channels = weights.shape[2]
    tokens = micro * per
    step = channels // slabs

    def kernel(ids_hbm, embed_hbm, weights_hbm, out_ref, embedded_ref, weights_ref, *rest):
        saved, (ids_ref, embed_ref, small, large) = rest[:4], rest[4:]
        first = [
            pltpu.make_async_copy(ids_hbm, ids_ref, small.at[0]),
            pltpu.make_async_copy(embed_hbm, embed_ref, small.at[1]),
        ]
        copies = {}
        for i in range(slabs):
            for m in (0, 1):
                part = pl.ds(i * step, step)
                copies[i, m] = pltpu.make_async_copy(
                    weights_hbm.at[m, :, part], weights_ref.at[m, :, part], large.at[2 * i + m]
                )

        @on_turn(0)
        def _():
            for copy in (*first, *(copies[i, 0] for i in range(slabs))):
                copy.start()
            for copy in first:
                copy.wait()
            for i in range(slabs):
                copies[i, 1].start()
            for m in range(micro):
                ids = ids_ref[m : m + 1, :]
                hot = (lax.broadcasted_iota(jnp.int32, (vocab, per), 0) == ids).astype(f32).astype(bf16)
                embedded_ref[m * per : (m + 1) * per, :] = down(hot, embed_ref[...]).astype(bf16)
            parts = [(pl.ds(i * step, step), lambda m, i=i: copies[i, m].wait()) for i in range(slabs)]
            block_on(embedded_ref[0:rows, :], parts, weights_ref, out_ref, saved, pl.ds(0, rows))

    got = call(
        kernel,
        [((rows, width), bf16), ((tokens, width), bf16), (weights.shape, bf16), *saved_shapes(tokens, width, channels)],
        [],
        read=[token_ids, embed, weights],
        flops=4 * rows * width * channels,
        scratch=[
            pltpu.VMEM(token_ids.shape, token_ids.dtype),
            pltpu.VMEM(embed.shape, embed.dtype),
            pltpu.SemaphoreType.DMA((2,)),
            pltpu.SemaphoreType.DMA((2 * slabs,)),
        ],
    )
    return got[0], got[1], got[2], got[3:]


def fetched(weights, held_weights):
    def kernel(weights_hbm, _, weights_ref, done):
        @pl.when(lax.axis_index("section") != 0)
        def _():
            copy = pltpu.make_async_copy(weights_hbm, weights_ref, done)
            copy.start()
            copy.wait()

    return call(
        kernel, [(weights.shape, bf16)], [held_weights], {1: 0}, read=[weights], scratch=[pltpu.SemaphoreType.DMA]
    )[0]


def forward(turn, inputs, weights, saved, start, rows, tokens, last):
    width = inputs.shape[1]
    channels = weights.shape[2]
    step = channels // slabs
    outs = saved_shapes(tokens, width, channels) + ([] if last else [((rows, width), bf16)])

    def kernel(x_ref, w_ref, *refs):
        refs = refs[len(saved) :]

        @on_turn(turn)
        def _():
            parts = [(pl.ds(i * step, step), lambda m: None) for i in range(slabs)]
            out_ref = None if last else refs[4]
            block_on(rows_of(x_ref, start, rows), parts, w_ref, out_ref, refs[:4], pl.ds(start, rows))

    got = call(
        kernel,
        outs,
        [inputs, weights, *saved],
        {2 + i: i for i in range(4)},
        flops=(2 if last else 4) * rows * width * channels,
        transcendentals=rows * channels,
    )
    return (None if last else got[4]), got[:4]


def backward(turn, grad, weights, saved, kept, start, rows, tokens, last):
    width = grad.shape[1]
    channels = weights.shape[2]
    step = channels // slabs
    outs = [((tokens, width), bf16), ((tokens, channels), bf16)]
    if not last:
        outs = outs + [((rows, width), bf16)]

    def kernel(grad_ref, w_ref, x_ref, slope_ref, *refs):
        refs = refs[len(kept) :]
        grad_out, upper_out = refs[:2]
        here = pl.ds(start, rows)

        @on_turn(turn)
        def _():
            grad = rows_of(grad_ref, start, rows)
            grad_out[here, :] = grad
            total = jnp.zeros((rows, width), f32)
            for i in range(slabs):
                part = pl.ds(i * step, step)
                back_hidden = jnp.dot(grad, w_ref[1, :, part], preferred_element_type=f32)
                back_upper = (back_hidden * slope_ref[here, part]).astype(bf16)
                upper_out[here, part] = back_upper
                if not last:
                    total = total + across(back_upper, w_ref[0, :, part])
            if not last:
                normed, scaled = normalize(x_ref[here, :])
                first = jnp.mean(total, axis=-1, keepdims=True)
                second = jnp.mean(total * normed, axis=-1, keepdims=True)
                refs[2][...] = (grad.astype(f32) + scaled * (total - first - normed * second)).astype(bf16)

    got = call(
        kernel,
        outs,
        [grad, weights, *saved, *kept],
        {4 + i: i for i in range(len(kept))},
        flops=(2 if last else 4) * rows * width * channels,
    )
    return (None if last else got[2]), got[:2]


def cut_up(tokens):
    count = chunk_count if tokens % 16 == 0 else 1
    units = tokens // 16 if count > 1 else 1
    lengths = [(units // count + (1 if c < units % count else 0)) * (tokens // units) for c in range(count)]
    return [(sum(lengths[:c]), lengths[c]) for c in range(count)]


def relay(token_ids, embed, weights, cotangent):
    count = lax.axis_size("section")
    tokens = token_ids.shape[0] * token_ids.shape[1]
    chunks = cut_up(tokens)
    width = embed.shape[1]
    saved, kept = [], []
    entered, embedded, here, saved = enter(token_ids, embed, weights, chunks[0][1])
    weights = fetched(weights, here)
    state = [embedded] * len(chunks)
    grads = [cotangent.reshape(tokens, width)] * len(chunks)

    def passed(array, source, target):
        return lax.ppermute(array, "section", [(source, target)])

    def back(hop, c):
        nonlocal kept
        out, kept = backward(hop, grads[c], weights, [saved[0], saved[3]], kept, *chunks[c], tokens, hop == 0)
        if hop:
            grads[c] = passed(out, hop, hop - 1)

    for hop in range(count):
        for c in range(len(chunks)):
            if hop or c:
                out, saved = forward(hop, state[c], weights, saved, *chunks[c], tokens, hop + 1 == count)
            else:
                out = entered
            if hop + 1 < count:
                state[c] = passed(out, hop, hop + 1)
            else:
                back(hop, c)
    for hop in range(count - 2, -1, -1):
        for c in range(len(chunks)):
            back(hop, c)
    return saved[1], saved[2], kept[0], kept[1], weights


def along(array, pairs):
    return lax.ppermute(array, "dp", [(2 * a + c, 2 * b + c) for a, b in pairs for c in (0, 1)])


def swapped(array):
    return lax.ppermute(array, "dp", [(i, i ^ 1) for i in range(lax.axis_size("dp"))])


def known_rows(error, known, parts, mine):
    owned, channels = parts[0][1].shape[-2:]

    def kernel(error_ref, *refs):
        outs = refs[len(known) + len(parts) :]
        z, core = place_on_line()
        for (chip, _, slot), ref in zip(parts, refs[len(known) :]):
            block = 2 * chip(z) + (core if mine else 1 - core)
            rows = pl.ds(pl.multiple_of(block * owned, owned), owned)
            values = ref[...] if mine else ref[slot]
            if mine:
                outs[1][slot] = values
            outs[0][block] = 0.9 * values.astype(f32) + error_ref[rows, :].astype(f32)

    return call(
        kernel,
        [((8, owned, channels), f32)] + ([((len(parts), owned, channels), bf16)] if mine else []),
        [error, *known, *[a for _, a, _ in parts]],
        {1: 0} if known else {},
    )


def add_gradient(known, normed, upper, grad, hidden):
    blocks, owned, channels = known.shape
    rows, width = normed.shape
    step = channels // 4
    per = blocks // 2

    def kernel(known_ref, normed_ref, upper_ref, grad_ref, hidden_ref, out_ref, sum_ref):
        total = jnp.zeros((8, step), f32)
        for m, (left, right) in enumerate(((normed_ref, upper_ref), (grad_ref, hidden_ref))):
            turned = left[...].T
            for c in range(channels // step):
                part = pl.ds(c * step, step)
                gradient = jnp.dot(turned, right[:, part], preferred_element_type=f32)
                for b in range(per):
                    block = m * per + b
                    combined = known_ref[block, :, part] + 0.1 * gradient[b * owned : (b + 1) * owned]
                    out_ref[block, :, part] = combined
                    total = total + jnp.sum((combined * combined).reshape(owned // 8, 8, step), axis=0)
        sum_ref[...] = jnp.broadcast_to(jnp.sum(total, axis=(0, 1), keepdims=True), sum_ref.shape)

    return call(
        kernel,
        [(known.shape, f32), ((8, 128), f32)],
        [known, normed, upper, grad, hidden],
        {0: 0},
        limit=12,
        flops=4 * rows * width * channels,
    )


def scale_of(sum_ref, count):
    scale = jnp.sqrt(sum_ref[0:1, 0:1] * (1.0 / count) + 0.01)
    return scale, 1.0 / scale


def chips_in_order(z):
    upper_half = z >> 1
    return (3 - 3 * upper_half, 2 - upper_half, z ^ 1, z)


def packed_part(sums, combined, places):
    blocks, owned, channels = combined.shape
    count = blocks * owned * channels

    def kernel(sum_ref, combined_ref, *outs):
        z, core = place_on_line()
        order = chips_in_order(z)
        scale, inverse = scale_of(sum_ref, count)
        for i, place in enumerate(places):
            for j, side in enumerate((1 - core, core)):
                values = combined_ref[2 * order[place] + side]
                outs[2 * i + j][...] = (scale * jnp.tanh(values * inverse)).astype(bf16)

    return call(
        kernel,
        [((owned, channels), bf16)] * (2 * len(places)),
        [sums, combined],
        transcendentals=2 * len(places) * owned * channels,
    )


def fresh_worker(sums, combined):
    blocks, owned, channels = combined.shape
    count = blocks * owned * channels

    def kernel(sum_ref, combined_ref, out_ref, made, done):
        scale, inverse = scale_of(sum_ref, count)
        copies = []
        for b in range(blocks):
            values = combined_ref[b]
            packed = (scale * jnp.tanh(values * inverse)).astype(bf16)
            made[b] = (values - packed.astype(f32)).astype(bf16)
            copies.append(pltpu.make_async_copy(made.at[b], out_ref.at[pl.ds(b * owned, owned), :], done.at[b]))
            copies[-1].start()
        for copy in copies:
            copy.wait()

    return call(
        kernel,
        [],
        [sums, combined],
        transcendentals=count,
        written=[((blocks * owned, channels), bf16)],
        scratch=[pltpu.VMEM((blocks, owned, channels), bf16), pltpu.SemaphoreType.DMA((blocks,))],
    )[0]


def added(cut, count, *arrays):
    rows, channels = arrays[0].shape[0] // count, arrays[0].shape[1]

    def kernel(*refs):
        total = jnp.zeros((rows, channels), f32)
        for ref in refs[:-1]:
            total = total + rows_of(ref, cut * rows, rows).astype(f32)
        refs[-1][...] = total.astype(bf16)

    return call(kernel, [((rows, channels), bf16)], list(arrays))[0]


def prepared(mine, other, error, variance, replicas):
    def kernel(mine_ref, other_ref, error_ref, variance_ref, base_ref, rate_ref):
        base_ref[...] = (mine_ref[...].astype(f32) + other_ref[...].astype(f32)) * (1.0 / replicas) + error_ref[...]
        rate_ref[...] = 0.01 / (jnp.sqrt(variance_ref[...].astype(f32)) + 1e-08)

    return call(kernel, [(error.shape, f32), (error.shape, f32)], [mine, other, error, variance])


def server(base, rate, parts, weights, replicas):
    owned, channels = base.shape
    per = weights.shape[1] // owned
    cuts = 4 if owned % 64 == 0 else 1
    rows = owned // cuts
    flat = [a for part in parts for a in part]

    def kernel(base_ref, rate_ref, weights_ref, *refs):
        got, outs, (merged_ref, w_made, m_made, e_made, done) = refs[:-8], refs[-8:-5], refs[-5:]
        squares = jnp.zeros((8, channels), f32)
        for i in range(cuts):
            here = pl.ds(i * rows, rows)
            total = jnp.zeros((rows, channels), f32)
            at = 0
            for part in parts:
                high = part[0].shape[0]
                total = total + got[at + i * rows // high][pl.ds(i * rows % high, rows), :].astype(f32)
                at += len(part)
            merged = total * (1.0 / replicas) + base_ref[here, :]
            merged_ref[here, :] = merged
            squares = squares + jnp.sum((merged * merged).reshape(rows // 8, 8, channels), axis=0)
        mean = jnp.sum(squares, axis=(0, 1), keepdims=True) * (1.0 / (owned * channels))
        scale = jnp.sqrt(mean + 0.01)
        inverse = 1.0 / scale
        rank = lax.axis_index("dp")
        matrix = jnp.where(rank >= per, 1, 0)
        first = (rank - per * matrix) * owned
        copies = []
        for i in range(cuts):
            here = pl.ds(i * rows, rows)
            merged = merged_ref[here, :]
            values = (scale * jnp.tanh(merged * inverse)).astype(bf16)
            m_made[here, :] = values
            wide = values.astype(f32)
            e_made[here, :] = merged - wide
            own = weights_ref[matrix, pl.ds(pl.multiple_of(first + i * rows, rows), rows), :].astype(f32)
            w_made[here, :] = (own - wide * rate_ref[here, :]).astype(bf16)
            for j, made in enumerate((w_made, m_made, e_made)):
                copies.append(pltpu.make_async_copy(made.at[here, :], outs[j].at[here, :], done.at[3 * i + j]))
                copies[-1].start()
        for copy in copies:
            copy.wait()

    shape = (owned, channels)
    return call(
        kernel,
        [],
        [base, rate, weights, *flat],
        transcendentals=owned * channels,
        written=[(shape, bf16), (shape, bf16), (shape, f32)],
        scratch=[
            pltpu.VMEM(shape, f32),
            pltpu.VMEM(shape, bf16),
            pltpu.VMEM(shape, bf16),
            pltpu.VMEM(shape, f32),
            pltpu.SemaphoreType.DMA((3 * cuts,)),
        ],
    )


def turned_round(own, inner):
    def kernel(own_ref, inner_ref, out_ref):
        z, _ = place_on_line()
        at_end = jnp.logical_or(z == 0, z == 3)
        for ref, here in ((own_ref, at_end), (inner_ref, jnp.logical_not(at_end))):

            @pl.when(here)
            def _(ref=ref):
                out_ref[...] = ref[...]

    return call(kernel, [(own.shape, own.dtype)], [own, inner])[0]


def on_a_line(token_ids, embed, weights, variance, momentum, error, server_error, cotangent):
    replicas = lax.axis_size("dp")
    inner = along(momentum, [(1, 2), (2, 1), (0, 3), (3, 0)])
    beside = along(momentum, [(0, 1), (1, 0), (2, 3), (3, 2)])
    onward = turned_round(momentum, inner)
    onward = along(onward, [(0, 2), (2, 3), (3, 1), (1, 0)])
    first = [(lambda z: z, momentum, 0), (lambda z: 3 - z, inner, 1), (lambda z: z ^ 1, beside, 2)]
    known, out_a = known_rows(error, [], first, True)
    in_a = swapped(out_a)
    known, out_b = known_rows(error, [known], [(lambda z: z ^ 2, onward, 0)], True)
    in_b = swapped(out_b)
    rest = [(chip, in_a, slot) for chip, _, slot in first] + [(lambda z: z ^ 2, in_b, 0)]
    known = known_rows(error, [known], rest, False)[0]
    normed, hidden, grad, upper, weights = relay(token_ids, embed, weights, cotangent)
    combined, sums = add_gradient(known, normed, upper, grad, hidden)
    far_out, far = packed_part(sums, combined, (0,))
    made = packed_part(sums, combined, (1, 2, 3))
    mine = {"far": far, "mid": made[1], "near": made[3], "own": made[5]}
    other = {}
    for name, out in (("far", far_out), ("mid", made[0]), ("near", made[2]), ("own", made[4])):
        other[name] = swapped(out)

    def summed(name, pairs, cut, count, *more):
        total = added(cut, count, mine[name], other[name], *more)
        return along(total, pairs)

    ends, inner, outer = [(0, 1), (3, 2)], [(1, 2), (2, 1)], [(2, 3), (1, 0)]
    both = range(halves)
    both_ways = [(0, 1), (1, 0), (2, 3), (3, 2)]
    a1 = [summed("far", ends if h else both_ways, h, halves) for h in both]
    a2 = [summed("mid", ends, h, halves) for h in both]
    a3 = [summed("near", ends, 0, 1)]
    b2 = [summed("far", inner, h, halves, a1[h]) for h in both]
    b3 = [summed("mid", inner, h, halves, a2[h]) for h in both]
    c3 = [summed("near", outer, h, halves, b2[h]) for h in both]
    new_worker = fresh_worker(sums, combined)
    base, rate = prepared(mine["own"], other["own"], server_error, variance, replicas)
    new_weights, new_momentum, new_server = server(base, rate, [a3, b3, c3], weights, replicas)
    return new_weights, new_momentum, new_worker, new_server


def in_general(token_ids, embed, weights, variance, momentum, error, server_error, cotangent):
    replicas = lax.axis_size("dp")
    width, channels = weights.shape[1:]
    owned = 2 * width // replicas
    shared = lax.all_gather(momentum, "dp", axis=0, tiled=True)
    normed, hidden, grad, upper, weights = relay(token_ids, embed, weights, cotangent)
    gradient = jnp.concatenate(
        [down(normed, upper), down(grad, hidden)], axis=0
    )
    combined = 0.9 * shared.astype(f32) + 0.1 * gradient + error.astype(f32)
    worker_scale = jnp.sqrt(jnp.mean(combined * combined) + 0.01)
    packed = (worker_scale * jnp.tanh(combined / worker_scale)).astype(bf16)
    new_worker = (combined - packed.astype(f32)).astype(bf16)
    total = lax.psum_scatter(packed.astype(f32), "dp", scatter_dimension=0, tiled=True)
    merged = total / replicas + server_error
    server_scale = jnp.sqrt(jnp.mean(merged * merged) + 0.01)
    values = (server_scale * jnp.tanh(merged / server_scale)).astype(bf16)
    wide = values.astype(f32)
    start = lax.axis_index("dp") * owned
    own = lax.dynamic_slice_in_dim(weights.reshape(2 * width, channels), start, owned, 0)
    step = 0.01 * wide / (jnp.sqrt(variance.astype(f32)) + 1e-08)
    return (own.astype(f32) - step).astype(bf16), values, new_worker, merged - wide


def local(token_ids, embed, weights, variance, momentum, worker_error, server_error, cotangent):
    _, _, width, channels = weights.shape
    plan = on_a_line if lax.axis_size("dp") == 8 else in_general
    new_weights, values, new_worker, new_server = plan(
        token_ids,
        embed,
        weights[0],
        variance[0],
        momentum[0],
        worker_error.reshape(2 * width, channels),
        server_error[0],
        cotangent,
    )
    return new_weights[None], values[None], new_worker.reshape(worker_error.shape), new_server[None]


def solution(mesh):
    in_specs = (
        P(None, "dp"),
        P(),
        P("section", None, None, None),
        P("section", "dp", None),
        P("section", "dp", None),
        P("section", "dp", None, None, None),
        P("section", "dp", None),
        P(None, "dp", None),
    )
    out_specs = (
        P("section", "dp", None),
        P("section", "dp", None),
        P("section", "dp", None, None, None),
        P("section", "dp", None),
    )
    return jax.shard_map(local, mesh=mesh, in_specs=in_specs, out_specs=out_specs, check_vma=False)
```

```python
import math

import jax
import jax.numpy as jnp
from jax import lax
from jax.experimental import pallas as pl
from jax.experimental.pallas import tpu as pltpu
from jax.sharding import PartitionSpec as P


gelu_coef = math.sqrt(2.0 / math.pi)
bf16, f32 = jnp.bfloat16, jnp.float32
whole = pl.BlockSpec(memory_space=pltpu.VMEM)
outside = pl.BlockSpec(memory_space=pl.ANY)


def held(array):
    return pltpu.with_memory_space_constraint(array, pltpu.VMEM)


def call(kernel, outs, arrays, aliases=None, limit=8, flops=0, transcendentals=0, written=(), scratch=(), read=()):
    moved = sum(math.prod(a.shape) * a.dtype.itemsize for a in arrays)
    return pl.pallas_call(
        kernel,
        out_shape=[pltpu.VMEM(shape, dtype) for shape, dtype in outs]
        + [jax.ShapeDtypeStruct(shape, dtype) for shape, dtype in written],
        in_specs=[outside] * len(read) + [whole] * len(arrays),
        out_specs=[whole] * len(outs) + [outside] * len(written),
        input_output_aliases=aliases or {},
        scratch_shapes=list(scratch),
        compiler_params=pltpu.CompilerParams(vmem_limit_bytes=limit << 20),
        cost_estimate=pl.CostEstimate(flops=flops, bytes_accessed=moved, transcendentals=transcendentals),
    )(*[pltpu.with_memory_space_constraint(a, pltpu.HBM) for a in read], *[held(a) for a in arrays])


def place_on_line():
    rank = lax.axis_index("dp")
    return rank >> 1, rank & 1


def across(left, right):
    return lax.dot_general(left, right, (((1,), (1,)), ((), ())), preferred_element_type=f32)


def down(left, right):
    return lax.dot_general(left, right, (((0,), (0,)), ((), ())), preferred_element_type=f32)


def normalize(inputs):
    values = inputs.astype(f32)
    center = jnp.mean(values, axis=-1, keepdims=True)
    shifted = values - center
    scaled = lax.rsqrt(jnp.mean(shifted * shifted, axis=-1, keepdims=True) + 1e-05)
    return shifted * scaled, scaled


slabs = 2
chunk_count = 2
halves = 2


def on_turn(turn):
    return pl.when(lax.axis_index("section") == turn)


def rows_of(ref, start, rows):
    return ref[...] if ref.shape[0] == rows else ref[start : start + rows, :]


def block_on(inputs, parts, weights_ref, out_ref, saved, place):
    x_out, normed_out, hidden_out, slope_out = saved
    normed_b = normalize(inputs)[0].astype(bf16)
    x_out[place, :] = inputs
    normed_out[place, :] = normed_b
    total = inputs.astype(f32) if out_ref is not None else None
    for part, ready in parts:
        ready(0)
        upper = jnp.dot(normed_b, weights_ref[0, :, part], preferred_element_type=f32)
        square = upper * upper
        bent = jnp.tanh(gelu_coef * upper * (1.0 + 0.044715 * square))
        half = 0.5 + 0.5 * bent
        hidden = (upper * half).astype(bf16)
        hidden_out[place, part] = hidden
        slope_out[place, part] = half + 0.5 * upper * (1.0 - bent * bent) * (
            gelu_coef * (1.0 + 3.0 * 0.044715 * square)
        )
        ready(1)
        if out_ref is not None:
            total = total + across(hidden, weights_ref[1, :, part])
    if out_ref is not None:
        out_ref[...] = total.astype(bf16)


def saved_shapes(tokens, width, channels):
    return [((tokens, width), bf16), ((tokens, width), bf16), ((tokens, channels), bf16), ((tokens, channels), f32)]


def enter(token_ids, embed, weights, rows):
    micro, per = token_ids.shape
    vocab, width = embed.shape
    channels = weights.shape[2]
    tokens = micro * per
    step = channels // slabs

    def kernel(ids_hbm, embed_hbm, weights_hbm, out_ref, embedded_ref, weights_ref, *rest):
        saved, (ids_ref, embed_ref, small, large) = rest[:4], rest[4:]
        first = [
            pltpu.make_async_copy(ids_hbm, ids_ref, small.at[0]),
            pltpu.make_async_copy(embed_hbm, embed_ref, small.at[1]),
        ]
        copies = {}
        for i in range(slabs):
            for m in (0, 1):
                part = pl.ds(i * step, step)
                copies[i, m] = pltpu.make_async_copy(
                    weights_hbm.at[m, :, part], weights_ref.at[m, :, part], large.at[2 * i + m]
                )

        @on_turn(0)
        def _():
            for copy in (*first, *(copies[i, 0] for i in range(slabs))):
                copy.start()
            for copy in first:
                copy.wait()
            for i in range(slabs):
                copies[i, 1].start()
            for m in range(micro):
                ids = ids_ref[m : m + 1, :]
                hot = (lax.broadcasted_iota(jnp.int32, (vocab, per), 0) == ids).astype(f32).astype(bf16)
                embedded_ref[m * per : (m + 1) * per, :] = down(hot, embed_ref[...]).astype(bf16)
            parts = [(pl.ds(i * step, step), lambda m, i=i: copies[i, m].wait()) for i in range(slabs)]
            block_on(embedded_ref[0:rows, :], parts, weights_ref, out_ref, saved, pl.ds(0, rows))

    got = call(
        kernel,
        [((rows, width), bf16), ((tokens, width), bf16), (weights.shape, bf16), *saved_shapes(tokens, width, channels)],
        [],
        read=[token_ids, embed, weights],
        flops=4 * rows * width * channels,
        scratch=[
            pltpu.VMEM(token_ids.shape, token_ids.dtype),
            pltpu.VMEM(embed.shape, embed.dtype),
            pltpu.SemaphoreType.DMA((2,)),
            pltpu.SemaphoreType.DMA((2 * slabs,)),
        ],
    )
    return got[0], got[1], got[2], got[3:]


def fetched(weights, held_weights, after):
    def kernel(weights_hbm, _, __, weights_ref, ___, done):
        @pl.when(lax.axis_index("section") != 0)
        def _():
            copy = pltpu.make_async_copy(weights_hbm, weights_ref, done)
            copy.start()
            copy.wait()

    return call(
        kernel,
        [(weights.shape, bf16), (after.shape, after.dtype)],
        [held_weights, after],
        {1: 0, 2: 1},
        read=[weights],
        scratch=[pltpu.SemaphoreType.DMA],
    )


def forward(turn, inputs, weights, saved, start, rows, tokens, last):
    width = inputs.shape[1]
    channels = weights.shape[2]
    step = channels // slabs
    outs = saved_shapes(tokens, width, channels) + ([] if last else [((rows, width), bf16)])

    def kernel(x_ref, w_ref, *refs):
        refs = refs[len(saved) :]

        @on_turn(turn)
        def _():
            parts = [(pl.ds(i * step, step), lambda m: None) for i in range(slabs)]
            out_ref = None if last else refs[4]
            block_on(rows_of(x_ref, start, rows), parts, w_ref, out_ref, refs[:4], pl.ds(start, rows))

    got = call(
        kernel,
        outs,
        [inputs, weights, *saved],
        {2 + i: i for i in range(4)},
        flops=(2 if last else 4) * rows * width * channels,
        transcendentals=rows * channels,
    )
    return (None if last else got[4]), got[:4]


def backward(turn, grad, weights, saved, kept, start, rows, tokens, last):
    width = grad.shape[1]
    channels = weights.shape[2]
    step = channels // slabs
    outs = [((tokens, width), bf16), ((tokens, channels), bf16)]
    if not last:
        outs = outs + [((rows, width), bf16)]

    def kernel(grad_ref, w_ref, x_ref, slope_ref, *refs):
        refs = refs[len(kept) :]
        grad_out, upper_out = refs[:2]
        here = pl.ds(start, rows)

        @on_turn(turn)
        def _():
            grad = rows_of(grad_ref, start, rows)
            grad_out[here, :] = grad
            total = jnp.zeros((rows, width), f32)
            for i in range(slabs):
                part = pl.ds(i * step, step)
                back_hidden = jnp.dot(grad, w_ref[1, :, part], preferred_element_type=f32)
                back_upper = (back_hidden * slope_ref[here, part]).astype(bf16)
                upper_out[here, part] = back_upper
                if not last:
                    total = total + across(back_upper, w_ref[0, :, part])
            if not last:
                normed, scaled = normalize(x_ref[here, :])
                first = jnp.mean(total, axis=-1, keepdims=True)
                second = jnp.mean(total * normed, axis=-1, keepdims=True)
                refs[2][...] = (grad.astype(f32) + scaled * (total - first - normed * second)).astype(bf16)

    got = call(
        kernel,
        outs,
        [grad, weights, *saved, *kept],
        {4 + i: i for i in range(len(kept))},
        flops=(2 if last else 4) * rows * width * channels,
    )
    return (None if last else got[2]), got[:2]


def cut_up(tokens):
    count = chunk_count if tokens % 16 == 0 else 1
    units = tokens // 16 if count > 1 else 1
    lengths = [(units // count + (1 if c < units % count else 0)) * (tokens // units) for c in range(count)]
    return [(sum(lengths[:c]), lengths[c]) for c in range(count)]


def relay(token_ids, embed, weights, cotangent):
    count = lax.axis_size("section")
    tokens = token_ids.shape[0] * token_ids.shape[1]
    chunks = cut_up(tokens)
    width = embed.shape[1]
    saved, kept = [], []
    entered, embedded, here, saved = enter(token_ids, embed, weights, chunks[0][1])
    elsewhere, weights = weights, here
    state = [embedded] * len(chunks)
    grads = [cotangent.reshape(tokens, width)] * len(chunks)

    def passed(array, source, target):
        return lax.ppermute(array, "section", [(source, target)])

    def back(hop, c):
        nonlocal kept
        out, kept = backward(hop, grads[c], weights, [saved[0], saved[3]], kept, *chunks[c], tokens, hop == 0)
        if hop:
            grads[c] = passed(out, hop, hop - 1)

    for hop in range(count):
        for c in range(len(chunks)):
            if hop or c:
                out, saved = forward(hop, state[c], weights, saved, *chunks[c], tokens, hop + 1 == count)
            else:
                out = entered
            if hop + 1 < count:
                state[c] = passed(out, hop, hop + 1)
            else:
                back(hop, c)
        if hop == 0:
            weights, first = fetched(elsewhere, weights, saved[0])
            saved = [first, *saved[1:]]
    for hop in range(count - 2, -1, -1):
        for c in range(len(chunks)):
            back(hop, c)
    return saved[1], saved[2], kept[0], kept[1], weights


def along(array, pairs):
    return lax.ppermute(array, "dp", [(2 * a + c, 2 * b + c) for a, b in pairs for c in (0, 1)])


def swapped(array):
    return lax.ppermute(array, "dp", [(i, i ^ 1) for i in range(lax.axis_size("dp"))])


def known_rows(error, known, parts, mine):
    owned, channels = parts[0][1].shape[-2:]

    def kernel(error_ref, *refs):
        outs = refs[len(known) + len(parts) :]
        z, core = place_on_line()
        for (chip, _, slot), ref in zip(parts, refs[len(known) :]):
            block = 2 * chip(z) + (core if mine else 1 - core)
            rows = pl.ds(pl.multiple_of(block * owned, owned), owned)
            values = ref[...] if mine else ref[slot]
            if mine:
                outs[1][slot] = values
            outs[0][block] = 0.9 * values.astype(f32) + error_ref[rows, :].astype(f32)

    return call(
        kernel,
        [((8, owned, channels), f32)] + ([((len(parts), owned, channels), bf16)] if mine else []),
        [error, *known, *[a for _, a, _ in parts]],
        {1: 0} if known else {},
    )


def add_gradient(known, normed, upper, grad, hidden):
    blocks, owned, channels = known.shape
    rows, width = normed.shape
    step = channels // 4
    per = blocks // 2

    def kernel(known_ref, normed_ref, upper_ref, grad_ref, hidden_ref, out_ref, sum_ref):
        total = jnp.zeros((8, step), f32)
        for m, (left, right) in enumerate(((normed_ref, upper_ref), (grad_ref, hidden_ref))):
            turned = left[...].T
            for c in range(channels // step):
                part = pl.ds(c * step, step)
                gradient = jnp.dot(turned, right[:, part], preferred_element_type=f32)
                for b in range(per):
                    block = m * per + b
                    combined = known_ref[block, :, part] + 0.1 * gradient[b * owned : (b + 1) * owned]
                    out_ref[block, :, part] = combined
                    total = total + jnp.sum((combined * combined).reshape(owned // 8, 8, step), axis=0)
        sum_ref[...] = jnp.broadcast_to(jnp.sum(total, axis=(0, 1), keepdims=True), sum_ref.shape)

    return call(
        kernel,
        [(known.shape, f32), ((8, 128), f32)],
        [known, normed, upper, grad, hidden],
        {0: 0},
        limit=12,
        flops=4 * rows * width * channels,
    )


def scale_of(sum_ref, count):
    scale = jnp.sqrt(sum_ref[0:1, 0:1] * (1.0 / count) + 0.01)
    return scale, 1.0 / scale


def chips_in_order(z):
    upper_half = z >> 1
    return (3 - 3 * upper_half, 2 - upper_half, z ^ 1, z)


def packed_part(sums, combined, places):
    blocks, owned, channels = combined.shape
    count = blocks * owned * channels

    def kernel(sum_ref, combined_ref, *outs):
        z, core = place_on_line()
        order = chips_in_order(z)
        scale, inverse = scale_of(sum_ref, count)
        for i, place in enumerate(places):
            for j, side in enumerate((1 - core, core)):
                values = combined_ref[2 * order[place] + side]
                outs[2 * i + j][...] = (scale * jnp.tanh(values * inverse)).astype(bf16)

    return call(
        kernel,
        [((owned, channels), bf16)] * (2 * len(places)),
        [sums, combined],
        transcendentals=2 * len(places) * owned * channels,
    )


def fresh_worker(sums, combined):
    blocks, owned, channels = combined.shape
    count = blocks * owned * channels

    def kernel(sum_ref, combined_ref, out_ref, made, done):
        scale, inverse = scale_of(sum_ref, count)
        copies = []
        for b in range(blocks):
            values = combined_ref[b]
            packed = (scale * jnp.tanh(values * inverse)).astype(bf16)
            made[b] = (values - packed.astype(f32)).astype(bf16)
            copies.append(pltpu.make_async_copy(made.at[b], out_ref.at[pl.ds(b * owned, owned), :], done.at[b]))
            copies[-1].start()
        for copy in copies:
            copy.wait()

    return call(
        kernel,
        [],
        [sums, combined],
        transcendentals=count,
        written=[((blocks * owned, channels), bf16)],
        scratch=[pltpu.VMEM((blocks, owned, channels), bf16), pltpu.SemaphoreType.DMA((blocks,))],
    )[0]


def added(cut, count, *arrays):
    rows, channels = arrays[0].shape[0] // count, arrays[0].shape[1]

    def kernel(*refs):
        total = jnp.zeros((rows, channels), f32)
        for ref in refs[:-1]:
            total = total + rows_of(ref, cut * rows, rows).astype(f32)
        refs[-1][...] = total.astype(bf16)

    return call(kernel, [((rows, channels), bf16)], list(arrays))[0]


def prepared(mine, other, error, variance, replicas):
    def kernel(mine_ref, other_ref, error_ref, variance_ref, base_ref, rate_ref):
        base_ref[...] = (mine_ref[...].astype(f32) + other_ref[...].astype(f32)) * (1.0 / replicas) + error_ref[...]
        rate_ref[...] = 0.01 / (jnp.sqrt(variance_ref[...].astype(f32)) + 1e-08)

    return call(kernel, [(error.shape, f32), (error.shape, f32)], [mine, other, error, variance])


def server(base, rate, parts, weights, replicas):
    owned, channels = base.shape
    per = weights.shape[1] // owned
    cuts = 4 if owned % 64 == 0 else 1
    rows = owned // cuts
    flat = [a for part in parts for a in part]

    def kernel(base_ref, rate_ref, weights_ref, *refs):
        got, outs, (merged_ref, w_made, m_made, e_made, done) = refs[:-8], refs[-8:-5], refs[-5:]
        squares = jnp.zeros((8, channels), f32)
        for i in range(cuts):
            here = pl.ds(i * rows, rows)
            total = jnp.zeros((rows, channels), f32)
            at = 0
            for part in parts:
                high = part[0].shape[0]
                total = total + got[at + i * rows // high][pl.ds(i * rows % high, rows), :].astype(f32)
                at += len(part)
            merged = total * (1.0 / replicas) + base_ref[here, :]
            merged_ref[here, :] = merged
            squares = squares + jnp.sum((merged * merged).reshape(rows // 8, 8, channels), axis=0)
        mean = jnp.sum(squares, axis=(0, 1), keepdims=True) * (1.0 / (owned * channels))
        scale = jnp.sqrt(mean + 0.01)
        inverse = 1.0 / scale
        rank = lax.axis_index("dp")
        matrix = jnp.where(rank >= per, 1, 0)
        first = (rank - per * matrix) * owned
        copies = []
        for i in range(cuts):
            here = pl.ds(i * rows, rows)
            merged = merged_ref[here, :]
            values = (scale * jnp.tanh(merged * inverse)).astype(bf16)
            m_made[here, :] = values
            wide = values.astype(f32)
            e_made[here, :] = merged - wide
            own = weights_ref[matrix, pl.ds(pl.multiple_of(first + i * rows, rows), rows), :].astype(f32)
            w_made[here, :] = (own - wide * rate_ref[here, :]).astype(bf16)
            for j, made in enumerate((w_made, m_made, e_made)):
                copies.append(pltpu.make_async_copy(made.at[here, :], outs[j].at[here, :], done.at[3 * i + j]))
                copies[-1].start()
        for copy in copies:
            copy.wait()

    shape = (owned, channels)
    return call(
        kernel,
        [],
        [base, rate, weights, *flat],
        transcendentals=owned * channels,
        written=[(shape, bf16), (shape, bf16), (shape, f32)],
        scratch=[
            pltpu.VMEM(shape, f32),
            pltpu.VMEM(shape, bf16),
            pltpu.VMEM(shape, bf16),
            pltpu.VMEM(shape, f32),
            pltpu.SemaphoreType.DMA((3 * cuts,)),
        ],
    )


def turned_round(own, inner):
    def kernel(own_ref, inner_ref, out_ref):
        z, _ = place_on_line()
        at_end = jnp.logical_or(z == 0, z == 3)
        for ref, here in ((own_ref, at_end), (inner_ref, jnp.logical_not(at_end))):

            @pl.when(here)
            def _(ref=ref):
                out_ref[...] = ref[...]

    return call(kernel, [(own.shape, own.dtype)], [own, inner])[0]


def on_a_line(token_ids, embed, weights, variance, momentum, error, server_error, cotangent):
    replicas = lax.axis_size("dp")
    inner = along(momentum, [(1, 2), (2, 1), (0, 3), (3, 0)])
    beside = along(momentum, [(0, 1), (1, 0), (2, 3), (3, 2)])
    onward = turned_round(momentum, inner)
    onward = along(onward, [(0, 2), (2, 3), (3, 1), (1, 0)])
    first = [(lambda z: z, momentum, 0), (lambda z: 3 - z, inner, 1), (lambda z: z ^ 1, beside, 2)]
    known, out_a = known_rows(error, [], first, True)
    in_a = swapped(out_a)
    known, out_b = known_rows(error, [known], [(lambda z: z ^ 2, onward, 0)], True)
    in_b = swapped(out_b)
    rest = [(chip, in_a, slot) for chip, _, slot in first] + [(lambda z: z ^ 2, in_b, 0)]
    known = known_rows(error, [known], rest, False)[0]
    normed, hidden, grad, upper, weights = relay(token_ids, embed, weights, cotangent)
    combined, sums = add_gradient(known, normed, upper, grad, hidden)
    far_out, far = packed_part(sums, combined, (0,))
    made = packed_part(sums, combined, (1, 2, 3))
    mine = {"far": far, "mid": made[1], "near": made[3], "own": made[5]}
    other = {}
    for name, out in (("far", far_out), ("mid", made[0]), ("near", made[2]), ("own", made[4])):
        other[name] = swapped(out)

    def summed(name, pairs, cut, count, *more):
        total = added(cut, count, mine[name], other[name], *more)
        return along(total, pairs)

    ends, inner, outer = [(0, 1), (3, 2)], [(1, 2), (2, 1)], [(2, 3), (1, 0)]
    both = range(halves)
    both_ways = [(0, 1), (1, 0), (2, 3), (3, 2)]
    a1 = [summed("far", ends if h else both_ways, h, halves) for h in both]
    a2 = [summed("mid", ends, h, halves) for h in both]
    a3 = [summed("near", ends, 0, 1)]
    b2 = [summed("far", inner, h, halves, a1[h]) for h in both]
    b3 = [summed("mid", inner, h, halves, a2[h]) for h in both]
    c3 = [summed("near", outer, h, halves, b2[h]) for h in both]
    new_worker = fresh_worker(sums, combined)
    base, rate = prepared(mine["own"], other["own"], server_error, variance, replicas)
    new_weights, new_momentum, new_server = server(base, rate, [a3, b3, c3], weights, replicas)
    return new_weights, new_momentum, new_worker, new_server


def in_general(token_ids, embed, weights, variance, momentum, error, server_error, cotangent):
    replicas = lax.axis_size("dp")
    width, channels = weights.shape[1:]
    owned = 2 * width // replicas
    shared = lax.all_gather(momentum, "dp", axis=0, tiled=True)
    normed, hidden, grad, upper, weights = relay(token_ids, embed, weights, cotangent)
    gradient = jnp.concatenate(
        [down(normed, upper), down(grad, hidden)], axis=0
    )
    combined = 0.9 * shared.astype(f32) + 0.1 * gradient + error.astype(f32)
    worker_scale = jnp.sqrt(jnp.mean(combined * combined) + 0.01)
    packed = (worker_scale * jnp.tanh(combined / worker_scale)).astype(bf16)
    new_worker = (combined - packed.astype(f32)).astype(bf16)
    total = lax.psum_scatter(packed.astype(f32), "dp", scatter_dimension=0, tiled=True)
    merged = total / replicas + server_error
    server_scale = jnp.sqrt(jnp.mean(merged * merged) + 0.01)
    values = (server_scale * jnp.tanh(merged / server_scale)).astype(bf16)
    wide = values.astype(f32)
    start = lax.axis_index("dp") * owned
    own = lax.dynamic_slice_in_dim(weights.reshape(2 * width, channels), start, owned, 0)
    step = 0.01 * wide / (jnp.sqrt(variance.astype(f32)) + 1e-08)
    return (own.astype(f32) - step).astype(bf16), values, new_worker, merged - wide


def local(token_ids, embed, weights, variance, momentum, worker_error, server_error, cotangent):
    _, _, width, channels = weights.shape
    plan = on_a_line if lax.axis_size("dp") == 8 else in_general
    new_weights, values, new_worker, new_server = plan(
        token_ids,
        embed,
        weights[0],
        variance[0],
        momentum[0],
        worker_error.reshape(2 * width, channels),
        server_error[0],
        cotangent,
    )
    return new_weights[None], values[None], new_worker.reshape(worker_error.shape), new_server[None]


def solution(mesh):
    in_specs = (
        P(None, "dp"),
        P(),
        P("section", None, None, None),
        P("section", "dp", None),
        P("section", "dp", None),
        P("section", "dp", None, None, None),
        P("section", "dp", None),
        P(None, "dp", None),
    )
    out_specs = (
        P("section", "dp", None),
        P("section", "dp", None),
        P("section", "dp", None, None, None),
        P("section", "dp", None),
    )
    return jax.shard_map(local, mesh=mesh, in_specs=in_specs, out_specs=out_specs, check_vma=False)
```
